128 devices in a mesh: dp: 1, tp: 2 (over core), ep: 64 (over z, y, x).
Axes of the slice: x: 4, y: 4, z: 4, core: 2. Of those that a mesh axis runs over, the one named last changes fastest.
Arguments:
- tokens: bfloat16 [65536, 2048], P(('dp', 'ep'))
- logits: float32 [65536, 128], P(('dp', 'ep'))
- w_up: bfloat16 [128, 2048, 768], P('ep', None, 'tp')
- w_down: bfloat16 [128, 768, 2048], P('ep', 'tp')
Outputs:
- output: bfloat16 [65536, 2048], P(('dp', 'ep'))
All inputs are finite; a program needn't handle non-finite values.
Results may differ from the reference program's by a relative error of at most 0.001.
Values are sent between devices in bfloat16 or wider.
A program may use at most 1 GiB of HBM per device.

```python
import jax
import jax.numpy as jnp
from jax import lax

N_TOKENS = 65536
N_SHARDS = 64
D_MODEL = 2048
D_FF = 768
N_EXPERTS = 128
CAPACITY = 1024

SHARD_LEN = N_TOKENS // N_SHARDS
SHARE = CAPACITY // N_SHARDS
HI_LEVELS = max(1, 4096 // CAPACITY)
LO_LEVELS = max(1, 4096 // (N_TOKENS - CAPACITY))


def draw_logits(key):
    k_shard, k_pair, k_local, k_order, k_high, k_low = jax.random.split(key, 6)
    half_shards = N_SHARDS // 2
    shard_base = jnp.broadcast_to(jnp.arange(N_SHARDS, dtype=jnp.int32), (N_EXPERTS, N_SHARDS))
    shard_perm = jax.random.permutation(k_shard, shard_base, axis=1, independent=True)
    pair_shift = jax.random.randint(k_pair, (N_EXPERTS, half_shards), 0, SHARE + 1)
    pair_shift = pair_shift.at[:, 0].set(SHARE)
    paired = jnp.concatenate([SHARE + pair_shift, SHARE - pair_shift], axis=1)
    expert_rows = jnp.arange(N_EXPERTS)[:, None]
    counts = jnp.zeros((N_EXPERTS, N_SHARDS), jnp.int32).at[expert_rows, shard_perm].set(paired)
    local_base = jnp.broadcast_to(jnp.arange(SHARD_LEN, dtype=jnp.int32), (N_EXPERTS, N_SHARDS, SHARD_LEN))
    local_rank = jax.random.permutation(k_local, local_base, axis=2, independent=True)
    chosen = (local_rank < counts[:, :, None]).reshape(N_EXPERTS, N_TOKENS)
    order_base = jnp.broadcast_to(jnp.arange(N_TOKENS, dtype=jnp.int32), (N_EXPERTS, N_TOKENS))
    order_perm = jax.random.permutation(k_order, order_base, axis=1, independent=True)
    sort_key = jnp.where(chosen, 0, N_TOKENS) + order_perm
    col_rank = jnp.argsort(jnp.argsort(sort_key, axis=1), axis=1).astype(jnp.int32)
    high_level = jax.random.randint(k_high, (N_EXPERTS, N_TOKENS), 0, HI_LEVELS)
    low_level = jax.random.randint(k_low, (N_EXPERTS, N_TOKENS), 0, LO_LEVELS)
    int_code = jnp.where(chosen, high_level * CAPACITY + col_rank, CAPACITY - 1 - col_rank - low_level * (N_TOKENS - CAPACITY))
    return int_code.T.astype(jnp.float32) / 1024.0


def setup_inputs(seed: int = 0, part: int = 0) -> dict:
    root_key = jax.random.key(seed)
    shared_key, part_base = jax.random.split(root_key)
    part_key = jax.random.fold_in(part_base, part)
    k_tokens, k_route = jax.random.split(part_key)
    k_up, k_down = jax.random.split(shared_key)
    tokens = jax.random.normal(k_tokens, (N_TOKENS, D_MODEL), jnp.float32).astype(jnp.bfloat16)
    w_up = (jax.random.normal(k_up, (N_EXPERTS, D_MODEL, D_FF), jnp.float32) * D_MODEL ** -0.5).astype(jnp.bfloat16)
    w_down = (jax.random.normal(k_down, (N_EXPERTS, D_FF, D_MODEL), jnp.float32) * (2.0 * D_FF ** -0.5)).astype(jnp.bfloat16)
    return {"tokens": tokens, "logits": draw_logits(k_route), "w_up": w_up, "w_down": w_down}


def reference(tokens, logits, w_up, w_down):
    gate_all = jax.nn.softmax(logits, axis=-1)
    chosen = lax.top_k(logits.T, CAPACITY)[1]

    def expert_ffn(operands):
        idx_e, up_e, down_e = operands
        picked = jnp.take(tokens, idx_e, axis=0)
        pre_act = jnp.dot(picked, up_e, preferred_element_type=jnp.float32)
        hidden = jax.nn.gelu(pre_act, approximate=True).astype(jnp.bfloat16)
        return jnp.dot(hidden, down_e, preferred_element_type=jnp.float32).astype(jnp.bfloat16)

    expert_out = lax.map(expert_ffn, (chosen, w_up, w_down))
    gate_sel = jnp.take_along_axis(gate_all.T, chosen, axis=1)
    contrib = expert_out.astype(jnp.float32) * gate_sel[:, :, None]
    mix_sum = jax.ops.segment_sum(contrib.reshape(-1, D_MODEL), chosen.reshape(-1), num_segments=N_TOKENS)
    return (tokens.astype(jnp.float32) + mix_sum).astype(jnp.bfloat16)
```

```python
import functools

import jax
import jax.numpy as jnp
import numpy as np
from jax import lax
from jax.experimental import pallas as pl
from jax.experimental.pallas import tpu as pltpu
from jax.sharding import PartitionSpec as P

CAP_FACTOR = 2
MESH = pl.DeviceIdType.MESH
SIDE = 4
WINDOW = 8
VMEM_LIMIT = 60 * 1024 * 1024


def neg(off):
    return tuple((-v) % SIDE for v in off)


def exchange_order():
    rest = [(a, b, c) for a in range(SIDE) for b in range(SIDE) for c in range(SIDE) if a or b or c]
    load = np.zeros(6)
    out = []

    def links(off):
        vec = np.zeros(6)
        for d, v in enumerate(off):
            if v in (1, 2):
                vec[2 * d] = 1
            if v in (2, 3):
                vec[2 * d + 1] = 1
        return vec

    while rest:
        best = min(rest, key=lambda o: (np.max(load + links(o)), np.sum((load + links(o)) ** 2) / (1 + links(o).sum())))
        rest.remove(best)
        out.append(best)
        load = (load + links(best)) * 0.8
    return out


ORDER = exchange_order()


def peer_of(me, core, off):
    pos = (me // (SIDE * SIDE), (me // SIDE) % SIDE, me % SIDE)
    z, y, x = (lax.rem(p + o + core * (2 * SIDE - 2 * o), SIDE) for p, o in zip(pos, off))
    return (z * SIDE + y) * SIDE + x


def route_kernel(n_cand, logit_ref, val_ref, idx_ref, gate_ref, work, soft):
    n_tok, lanes = logit_ref.shape
    step = 64
    best = jnp.full((8, lanes), -jnp.inf, jnp.float32)
    for lo in range(0, n_tok, step):
        v = logit_ref[lo:lo + step, :]
        e = jnp.exp(v - jnp.max(v, axis=1, keepdims=True))
        soft[lo:lo + step, :] = e / jnp.sum(e, axis=1, keepdims=True)
        work[lo:lo + step, :] = v
        best = jnp.maximum(best, jnp.max(v.reshape(step // 8, 8, lanes), axis=0))
    row = lax.broadcasted_iota(jnp.int32, (step, lanes), 0).astype(jnp.float32)

    def body(k, best):
        top = jnp.max(best, axis=0, keepdims=True)
        nxt = jnp.full((8, lanes), -jnp.inf, jnp.float32)
        pos = jnp.zeros((8, lanes), jnp.float32)
        gat = jnp.zeros((8, lanes), jnp.float32)
        for lo in range(0, n_tok, step):
            v = work[lo:lo + step, :]
            hit = v == top
            v = jnp.where(hit, -jnp.inf, v)
            work[lo:lo + step, :] = v
            nxt = jnp.maximum(nxt, jnp.max(v.reshape(step // 8, 8, lanes), axis=0))
            pos = pos + jnp.sum(jnp.where(hit, row + float(lo), 0.0).reshape(step // 8, 8, lanes), axis=0)
            gat = gat + jnp.sum(jnp.where(hit, soft[lo:lo + step, :], 0.0).reshape(step // 8, 8, lanes), axis=0)
        val_ref[pl.ds(k, 1), :] = top
        idx_ref[pl.ds(k, 1), :] = jnp.sum(pos, axis=0, keepdims=True).astype(jnp.int32)
        gate_ref[pl.ds(k, 1), :] = jnp.sum(gat, axis=0, keepdims=True)
        return nxt

    lax.fori_loop(0, n_cand, body, best)


def pick_kernel(idx_ref, x_ref, out_ref):
    rows = idx_ref.shape[0]
    n_tok = x_ref.shape[0]
    onehot = (lax.broadcasted_iota(jnp.int32, (rows, n_tok), 1) == idx_ref[...]).astype(jnp.bfloat16)
    out_ref[...] = jnp.dot(onehot, x_ref[...], preferred_element_type=jnp.float32).astype(jnp.bfloat16)


def run_window(copies):
    for j, c in enumerate(copies):
        if j >= WINDOW:
            copies[j - WINDOW].wait()
        c.start()
    for c in copies[-WINDOW:]:
        c.wait()


def dispatch_kernel(rows_ref, val_ref, wu_ref, wd_ref, rrows_ref, rval_ref, wup_ref, wdp_ref, send, recv, vsend, vrecv, wsend, wrecv, loc):
    me, core = lax.axis_index("ep"), lax.axis_index("tp")
    other = 1 - core
    weights = [
        pltpu.make_async_remote_copy(src.at[other], dst, wsend.at[i], wrecv.at[i], device_id={"tp": other}, device_id_type=MESH)
        for i, (src, dst) in enumerate(((wu_ref, wup_ref), (wd_ref, wdp_ref)))
    ]
    own = [pltpu.make_async_copy(rows_ref.at[me], rrows_ref.at[me], loc.at[0]), pltpu.make_async_copy(val_ref.at[me], rval_ref.at[me], loc.at[1])]
    copies, vals = [], []
    for j, off in enumerate(ORDER):
        to = peer_of(me, core, off)
        copies.append(pltpu.make_async_remote_copy(rows_ref.at[to], rrows_ref.at[me], send.at[j], recv.at[j], device_id={"ep": to}, device_id_type=MESH))
        vals.append(pltpu.make_async_remote_copy(val_ref.at[to], rval_ref.at[me], vsend.at[j], vrecv.at[j], device_id={"ep": to}, device_id_type=MESH))
    for c in own + weights + vals:
        c.start()
    run_window(copies)
    for c in own + weights + vals:
        c.wait()


def expert_kernel(capacity, core_ref, vcol_ref, vrow_ref, x_ref, wu_ref, wup_ref, wd_ref, wdp_ref, out_ref):
    x = x_ref[...]
    above = (vrow_ref[...] > vcol_ref[...]).astype(jnp.float32)
    keep = jnp.sum(above, axis=1, keepdims=True) < float(capacity)
    z = None
    for up, down in ((wu_ref[0], wd_ref[0]), (wup_ref[...], wdp_ref[...])):
        pre = jnp.dot(x, up, preferred_element_type=jnp.float32)
        hid = jax.nn.gelu(pre, approximate=True).astype(jnp.bfloat16)
        part = jnp.dot(hid, down, preferred_element_type=jnp.float32)
        z = part if z is None else z + part
    out_ref[...] = jnp.where(keep, z, 0.0).astype(jnp.bfloat16)


def return_kernel(z_ref, ret_ref, send, recv, loc):
    me, core = lax.axis_index("ep"), lax.axis_index("tp")
    half = z_ref.shape[2] // 2
    part = [z_ref.at[:, :, pl.ds(pl.multiple_of(h * half, half), half)] for h in (core, 1 - core)]
    own = pltpu.make_async_copy(part[0].at[me], ret_ref.at[me, core], loc)
    copies = [pltpu.make_async_remote_copy(part[1].at[me], ret_ref.at[me, core], send.at[0], recv.at[0], device_id={"tp": 1 - core}, device_id_type=MESH)]
    for j, off in enumerate(ORDER):
        to = peer_of(me, core, off)
        for h in range(2):
            sem = 1 + 2 * j + h
            copies.append(pltpu.make_async_remote_copy(part[h].at[to], ret_ref.at[me, core], send.at[sem], recv.at[sem], device_id={"tp": (core + h) % 2, "ep": to}, device_id_type=MESH))
    own.start()
    for j, c in enumerate(copies):
        if j >= 2 * WINDOW:
            copies[j - 2 * WINDOW].wait()
        c.start()
    for c in copies[-2 * WINDOW:]:
        c.wait()
    own.wait()


def combine_kernel(core_ref, idx_ref, gate_ref, z_ref, x_ref, out_ref, acc):
    step = pl.program_id(0)
    n_tok = x_ref.shape[0]
    rows = z_ref.shape[0]
    hit = lax.broadcasted_iota(jnp.int32, (n_tok, rows), 0) == idx_ref[...]
    left = gate_ref[...]
    total = None
    z = z_ref[...]
    for _ in range(3):
        piece = left.astype(jnp.bfloat16)
        left = left - piece.astype(jnp.float32)
        mat = jnp.where(hit, piece.astype(jnp.float32), 0.0).astype(jnp.bfloat16)
        part = jnp.dot(mat, z, preferred_element_type=jnp.float32)
        total = part if total is None else total + part

    @pl.when(step == 0)
    def _():
        acc[...] = total

    @pl.when(step > 0)
    def _():
        acc[...] += total

    @pl.when(step == pl.num_programs(0) - 1)
    def _():
        out_ref[...] = (x_ref[...].astype(jnp.float32) + acc[...]).astype(jnp.bfloat16)


def solution(mesh):
    n_groups = mesh.shape["ep"]
    any_spec = pl.BlockSpec(memory_space=pl.ANY)
    dma = pltpu.SemaphoreType.DMA
    n_off = len(ORDER)
    side_effects = pltpu.CompilerParams(has_side_effects=True)

    def local_layer(x_local, logit_local, w_up, w_down):
        n_tok, d_model = x_local.shape
        n_experts = logit_local.shape[1]
        own_experts, _, hid = w_up.shape
        capacity = CAP_FACTOR * n_tok * n_groups // n_experts
        cand = 2 * capacity // n_groups
        rows = n_groups * cand
        half = d_model // 2
        core = lax.axis_index("tp")
        core_arr = core.reshape(1).astype(jnp.int32)

        small = lambda dt: jax.ShapeDtypeStruct((cand, n_experts), dt)
        val, idx, gate = pl.pallas_call(
            functools.partial(route_kernel, cand),
            out_shape=(small(jnp.float32), small(jnp.int32), small(jnp.float32)),
            scratch_shapes=[pltpu.VMEM((n_tok, n_experts), jnp.float32), pltpu.VMEM((n_tok, n_experts), jnp.float32)],
        )(logit_local)
        mine = lambda a: lax.dynamic_index_in_dim(a.T.reshape(n_groups, own_experts, cand), core, 1, keepdims=False)
        val_send = jnp.pad(mine(val), ((0, 0), (0, 128 - cand))).reshape(n_groups, 1, 128)
        pick_idx = mine(idx).reshape(rows, 1)

        blk = 256
        send_rows = pl.pallas_call(
            pick_kernel,
            out_shape=jax.ShapeDtypeStruct((rows, d_model), jnp.bfloat16),
            grid=(rows // blk,),
            in_specs=[pl.BlockSpec((blk, 1), lambda i: (i, 0)), pl.BlockSpec((n_tok, d_model), lambda i: (0, 0))],
            out_specs=pl.BlockSpec((blk, d_model), lambda i: (i, 0)),
            compiler_params=pltpu.CompilerParams(vmem_limit_bytes=VMEM_LIMIT),
        )(pick_idx, x_local).reshape(n_groups, cand, d_model)

        recv_rows, recv_val, wu_peer, wd_peer = pl.pallas_call(
            dispatch_kernel,
            out_shape=(
                jax.ShapeDtypeStruct((n_groups, cand, d_model), jnp.bfloat16),
                jax.ShapeDtypeStruct((n_groups, 1, 128), jnp.float32),
                jax.ShapeDtypeStruct(w_up.shape[1:], jnp.bfloat16),
                jax.ShapeDtypeStruct(w_down.shape[1:], jnp.bfloat16),
            ),
            in_specs=[any_spec] * 4,
            out_specs=(any_spec,) * 4,
            scratch_shapes=[dma((n_off,)), dma((n_off,)), dma((n_off,)), dma((n_off,)), dma((2,)), dma((2,)), dma((2,))],
            compiler_params=side_effects,
        )(send_rows, val_send, w_up, w_down)

        cand_val = recv_val[:, 0, :cand].reshape(rows)
        z = pl.pallas_call(
            functools.partial(expert_kernel, capacity),
            out_shape=jax.ShapeDtypeStruct((rows, d_model), jnp.bfloat16),
            grid_spec=pltpu.PrefetchScalarGridSpec(
                num_scalar_prefetch=1,
                grid=(rows // blk,),
                in_specs=[
                    pl.BlockSpec((blk, 1), lambda i, c: (i, 0)),
                    pl.BlockSpec((1, rows), lambda i, c: (0, 0)),
                    pl.BlockSpec((blk, d_model), lambda i, c: (i, 0)),
                    pl.BlockSpec((1, d_model, hid), lambda i, c: (c[0], 0, 0)),
                    pl.BlockSpec((d_model, hid), lambda i, c: (0, 0)),
                    pl.BlockSpec((1, hid, d_model), lambda i, c: (c[0], 0, 0)),
                    pl.BlockSpec((hid, d_model), lambda i, c: (0, 0)),
                ],
                out_specs=pl.BlockSpec((blk, d_model), lambda i, c: (i, 0)),
            ),
            compiler_params=pltpu.CompilerParams(vmem_limit_bytes=VMEM_LIMIT),
        )(core_arr, cand_val.reshape(rows, 1), cand_val.reshape(1, rows), recv_rows.reshape(rows, d_model), w_up, wu_peer, w_down, wd_peer)

        ret = pl.pallas_call(
            return_kernel,
            out_shape=jax.ShapeDtypeStruct((n_groups, own_experts, cand, half), jnp.bfloat16),
            in_specs=[any_spec],
            out_specs=any_spec,
            scratch_shapes=[dma((2 * n_off + 1,)), dma((2 * n_off + 1,)), dma],
            compiler_params=side_effects,
        )(z.reshape(n_groups, cand, d_model))

        slots = n_experts * cand
        kblk = 512
        out_half = pl.pallas_call(
            combine_kernel,
            out_shape=jax.ShapeDtypeStruct((n_tok, half), jnp.bfloat16),
            grid_spec=pltpu.PrefetchScalarGridSpec(
                num_scalar_prefetch=1,
                grid=(slots // kblk,),
                in_specs=[
                    pl.BlockSpec((1, kblk), lambda i, c: (0, i)),
                    pl.BlockSpec((1, kblk), lambda i, c: (0, i)),
                    pl.BlockSpec((kblk, half), lambda i, c: (i, 0)),
                    pl.BlockSpec((n_tok, half), lambda i, c: (0, c[0])),
                ],
                out_specs=pl.BlockSpec((n_tok, half), lambda i, c: (0, 0)),
                scratch_shapes=[pltpu.VMEM((n_tok, half), jnp.float32)],
            ),
            compiler_params=pltpu.CompilerParams(vmem_limit_bytes=VMEM_LIMIT),
        )(core_arr, idx.T.reshape(1, slots), gate.T.reshape(1, slots), ret.reshape(slots, half), x_local)
        return lax.all_gather(out_half, "tp", axis=1, tiled=True)

    token_spec = P(("dp", "ep"), None)
    return jax.shard_map(local_layer, mesh=mesh, in_specs=(token_spec, token_spec, P("ep", None, "tp"), P("ep", "tp", None)), out_specs=token_spec, check_vma=False)
```

```python
import functools

import jax
import jax.numpy as jnp
from jax import lax
from jax.experimental import pallas as pl
from jax.experimental.pallas import tpu as pltpu
from jax.sharding import PartitionSpec as P

CAP_FACTOR = 2
MESH = pl.DeviceIdType.MESH
SIDE = 4
LAG = 2.0
EARLY = 2.0
AHEAD = 4.0
VMEM_LIMIT = 62 * 1024 * 1024
SELF = (0, 0, 0)


def neg(off):
    return tuple((-v) % SIDE for v in off)


def plan(lag):
    jobs = [(a, b, c) for a in range(SIDE) for b in range(SIDE) for c in range(SIDE) if a or b or c]
    dur = {1: 1.0, 3: 1.0, 2: 2.0}
    rem = {o: {d for d in range(3) if o[d]} for o in jobs}
    ready = {o: 0.0 for o in jobs}
    count = {o: 0 for o in jobs}
    free = [0.0] * 3
    legs = []
    while any(rem.values()):
        d = min((d for d in range(3) if any(d in rem[o] for o in jobs)), key=lambda d: free[d])
        cand = [o for o in jobs if d in rem[o]]
        avail = [o for o in cand if ready[o] <= free[d] + 1e-9]
        if not avail:
            free[d] = min(ready[o] for o in cand)
            continue
        o = min(avail, key=lambda o: (-len(rem[o]), -sum(dur[o[q]] for q in rem[o]), sum(o[q] * (7, 3, 5)[q] for q in range(3)) % 11, o))
        rem[o].discard(d)
        legs.append((free[d], o, d, count[o]))
        count[o] += 1
        free[d] += dur[o[d]]
        ready[o] = free[d] + lag
    return sorted(legs), {o: ready[o] - lag for o in jobs}, count


LEGS, FINISH, N_LEGS = plan(LAG)
START = {o: t for t, o, _, i in LEGS if i == 0}
LEG_ID = {(o, i): k for k, (_, o, _, i) in enumerate(LEGS)}
JOB_ID = {o: j for j, o in enumerate(sorted(FINISH))}
SEND_ORDER = sorted(FINISH, key=lambda o: (START[o], o)) + [SELF]
DONE_ORDER = [SELF] + sorted(FINISH, key=lambda o: (FINISH[o], o))
SEND_SLOT = {o: p for p, o in enumerate(SEND_ORDER)}
DONE_SLOT = {o: r for r, o in enumerate(DONE_ORDER)}
FINISH_ALL = {SELF: 0.0, **FINISH}


def peer_at(me, core, off):
    pos = (me // (SIDE * SIDE), (me // SIDE) % SIDE, me % SIDE)
    z, y, x = (lax.rem(p + o + core * (2 * SIDE - 2 * o), SIDE) for p, o in zip(pos, off))
    return (z * SIDE + y) * SIDE + x


def leg_peer(me, core, off, axis):
    return peer_at(me, core, tuple(v if q == axis else 0 for q, v in enumerate(off)))


def leg_time(leg):
    t, _, _, i = leg
    return t - (EARLY if i == 0 else 0.0)


def group_events(compute_times):
    groups, rest = [], sorted(LEGS, key=lambda leg: (leg_time(leg), leg))
    for t in compute_times:
        groups.append([leg for leg in rest if leg_time(leg) < t])
        rest = [leg for leg in rest if leg_time(leg) >= t]
    return groups + [rest]


def lane_column(table, lane):
    lanes = lax.broadcasted_iota(jnp.int32, table.shape, 1)
    return jnp.sum(jnp.where(lanes == lane, table, 0.0), axis=1, keepdims=True)


def route_kernel(n_cand, logit_ref, val_ref, idx_ref, gate_ref, work, soft):
    n_tok, lanes = logit_ref.shape
    step = 64
    best = jnp.full((8, lanes), -jnp.inf, jnp.float32)
    for lo in range(0, n_tok, step):
        v = logit_ref[lo:lo + step, :]
        e = jnp.exp(v - jnp.max(v, axis=1, keepdims=True))
        soft[lo:lo + step, :] = e / jnp.sum(e, axis=1, keepdims=True)
        work[lo:lo + step, :] = v
        best = jnp.maximum(best, jnp.max(v.reshape(step // 8, 8, lanes), axis=0))
    row = lax.broadcasted_iota(jnp.int32, (step, lanes), 0).astype(jnp.float32)

    def body(k, best):
        top = jnp.max(best, axis=0, keepdims=True)
        nxt = jnp.full((8, lanes), -jnp.inf, jnp.float32)
        pos = jnp.zeros((8, lanes), jnp.float32)
        gat = jnp.zeros((8, lanes), jnp.float32)
        for lo in range(0, n_tok, step):
            v = work[lo:lo + step, :]
            hit = v == top
            v = jnp.where(hit, -jnp.inf, v)
            work[lo:lo + step, :] = v
            nxt = jnp.maximum(nxt, jnp.max(v.reshape(step // 8, 8, lanes), axis=0))
            pos = pos + jnp.sum(jnp.where(hit, row + float(lo), 0.0).reshape(step // 8, 8, lanes), axis=0)
            gat = gat + jnp.sum(jnp.where(hit, soft[lo:lo + step, :], 0.0).reshape(step // 8, 8, lanes), axis=0)
        val_ref[pl.ds(k, 1), :] = top
        idx_ref[pl.ds(k, 1), :] = jnp.sum(pos, axis=0, keepdims=True)
        gate_ref[pl.ds(k, 1), :] = jnp.sum(gat, axis=0, keepdims=True)
        return nxt

    lax.fori_loop(0, n_cand, body, best)


def expert_kernel(capacity, idx_ref, x_ref, val_ref, wu_ref, wd_ref, z_ref,
                  cols, outbox, hop1, hop2, inbox, rval, wu, wd, zbuf, send, recv, vsend, vrecv, wsend, wrecv, lsem, zsem):
    me, core = lax.axis_index("ep"), lax.axis_index("tp")
    other = 1 - core
    n_slot, cand, d_model = outbox.shape
    n_tok, lanes = x_ref.shape[0], val_ref.shape[2]
    per = 8
    rows = per * cand
    n_chunk = n_slot // per
    hops = (hop1, hop2)
    own_experts = wu_ref.shape[0]

    weights = []
    for i, (src, dst) in enumerate(((wu_ref, wu), (wd_ref, wd))):
        weights.append(pltpu.make_async_copy(src.at[core], dst.at[0], lsem.at[i]))
        weights.append(pltpu.make_async_remote_copy(src.at[other], dst.at[1], wsend.at[i], wrecv.at[i], device_id={"tp": other}, device_id_type=MESH))
    own_val = pltpu.make_async_copy(val_ref.at[own_experts * me + core], rval.at[DONE_SLOT[SELF]], lsem.at[2])

    def val_copy(o):
        to = peer_at(me, core, o)
        j = JOB_ID[o]
        return pltpu.make_async_remote_copy(val_ref.at[own_experts * to + core], rval.at[DONE_SLOT[o]], vsend.at[j], vrecv.at[j], device_id={"ep": to}, device_id_type=MESH)

    def leg_copy(o, axis, i):
        last = i == N_LEGS[o] - 1
        src = outbox.at[SEND_SLOT[o]] if i == 0 else hops[i - 1].at[JOB_ID[o]]
        dst = inbox.at[DONE_SLOT[o]] if last else hops[i].at[JOB_ID[o]]
        k = LEG_ID[o, i]
        return pltpu.make_async_remote_copy(src, dst, send.at[k], recv.at[k], device_id={"ep": leg_peer(me, core, o, axis)}, device_id_type=MESH)

    def arrival(o, i):
        return pltpu.make_async_remote_copy(inbox.at[0], inbox.at[0], send.at[0], recv.at[LEG_ID[o, i]], device_id={"tp": other}, device_id_type=MESH)

    def run_legs(legs):
        for _, o, axis, i in legs:
            if i:
                arrival(o, i - 1).wait_recv()
            leg_copy(o, axis, i).start()

    idx = idx_ref[...]

    def set_columns(p):
        o = SEND_ORDER[p]
        cols[p * cand:(p + 1) * cand, :] = lane_column(idx, own_experts * peer_at(me, core, o) + core)

    pick_times = [min(leg_time((START[o], o, 0, 0)) for o in SEND_ORDER[g * per:(g + 1) * per] if o != SELF) - AHEAD for g in range(n_chunk)]
    done_times = [max(FINISH_ALL[o] for o in DONE_ORDER[g * per:(g + 1) * per]) + LAG for g in range(n_chunk)]
    groups = group_events(pick_times + done_times)

    for p in range(per):
        set_columns(p)

    def pick(g, c):
        for k in range(n_chunk):
            @pl.when(g == k)
            def _():
                run_legs(groups[k])
        at = pl.multiple_of(g * rows, rows)
        onehot = (lax.broadcasted_iota(jnp.int32, (rows, n_tok), 1).astype(jnp.float32) == cols[pl.ds(at, rows), :]).astype(jnp.bfloat16)
        got = jnp.dot(onehot, x_ref[...], preferred_element_type=jnp.float32).astype(jnp.bfloat16)
        outbox[pl.ds(g * per, per)] = got.reshape(per, cand, d_model)

        @pl.when(g == 0)
        def _():
            for c in weights + [own_val]:
                c.start()
            for o in FINISH:
                val_copy(o).start()
            for p in range(per, n_slot):
                set_columns(p)
        return c

    lax.fori_loop(0, n_chunk, pick, 0)
    inbox[DONE_SLOT[SELF]] = outbox[SEND_SLOT[SELF]]

    def expert(g, c):
        for k in range(n_chunk):
            @pl.when(g == k)
            def _():
                run_legs(groups[n_chunk + k])
                if k == 0:
                    for o in FINISH:
                        val_copy(o).wait_recv()
                    for c in weights + [own_val]:
                        c.wait()
                for o in DONE_ORDER[k * per:(k + 1) * per]:
                    if o != SELF:
                        arrival(o, N_LEGS[o] - 1).wait_recv()
                if k == n_chunk - 1:
                    run_legs(groups[2 * n_chunk])
        eye = lax.broadcasted_iota(jnp.int32, (cand, lanes), 0) == lax.broadcasted_iota(jnp.int32, (cand, lanes), 1)
        mine = jnp.concatenate([jnp.sum(jnp.where(eye, rval[g * per + i], 0.0), axis=1, keepdims=True) for i in range(per)], axis=0)
        pad = lax.broadcasted_iota(jnp.int32, (1, lanes), 1) < cand

        def count(j, acc):
            return acc + (jnp.where(pad, rval[j], -jnp.inf) > mine).astype(jnp.float32)

        above = lax.fori_loop(0, n_slot, count, jnp.zeros((rows, lanes), jnp.float32), unroll=8)
        keep = jnp.sum(above, axis=1, keepdims=True) < float(capacity)
        x = inbox[pl.ds(g * per, per)].reshape(rows, d_model)
        z = None
        for h in range(2):
            pre = jnp.dot(x, wu[h], preferred_element_type=jnp.float32)
            hid = jax.nn.gelu(pre, approximate=True).astype(jnp.bfloat16)
            part = jnp.dot(hid, wd[h], preferred_element_type=jnp.float32)
            z = part if z is None else z + part
        slot = lax.rem(g, 2)

        def flush(g, slot):
            return pltpu.make_async_copy(zbuf.at[slot], z_ref.at[pl.ds(g * per, per)], zsem.at[slot])

        @pl.when(g >= 2)
        def _():
            flush(g - 2, slot).wait()
        zbuf[slot] = jnp.where(keep, z, 0.0).astype(jnp.bfloat16).reshape(per, cand, d_model)
        flush(g, slot).start()

        @pl.when(g == n_chunk - 1)
        def _():
            flush(g - 1, 1 - slot).wait()
            flush(g, slot).wait()
        return c

    lax.fori_loop(0, n_chunk, expert, 0)

    def drain(k, c):
        pltpu.make_async_remote_copy(inbox.at[0], inbox.at[0], send.at[k], recv.at[0], device_id={"tp": other}, device_id_type=MESH).wait_send()
        return c

    lax.fori_loop(0, len(LEGS), drain, 0)

    def vdrain(k, c):
        pltpu.make_async_remote_copy(rval.at[0], rval.at[0], vsend.at[k], vrecv.at[0], device_id={"tp": other}, device_id_type=MESH).wait_send()
        return c

    lax.fori_loop(0, len(FINISH), vdrain, 0)


def combine_kernel(idx_ref, gate_ref, x_ref, z_ref, out_ref,
                   ids, gts, hop1, hop2, back, acc, xh, obuf, send, recv, asend, arecv, bsend, brecv, lsem, osend, orecv, osem):
    me, core = lax.axis_index("ep"), lax.axis_index("tp")
    other = 1 - core
    n_slot, n_par, cand, half = back.shape
    n_tok = x_ref.shape[0]
    per = 4
    rows = per * n_par * cand
    n_chunk = n_slot // per
    hops = (hop1, hop2)
    mine = pl.ds(pl.multiple_of(core * half, half), half)
    theirs = pl.ds(pl.multiple_of(other * half, half), half)

    def source(o, i):
        return z_ref.at[DONE_SLOT[neg(o)]] if i == 0 else hops[i - 1].at[JOB_ID[o]]

    def last_copies(o, src, to):
        j = DONE_SLOT[o]
        dst = back.at[j, core]
        same = None if to is None else pltpu.make_async_remote_copy(src.at[:, mine], dst, asend.at[j], arecv.at[j], device_id={"ep": to}, device_id_type=MESH)
        there = {"tp": other} if to is None else {"tp": other, "ep": to}
        cross = pltpu.make_async_remote_copy(src.at[:, theirs], dst, bsend.at[j], brecv.at[j], device_id=there, device_id_type=MESH)
        return same, cross

    def dummy(s, r):
        return pltpu.make_async_remote_copy(back.at[0, 0], back.at[0, 0], s, r, device_id={"tp": other}, device_id_type=MESH)

    def full(s, r):
        return pltpu.make_async_remote_copy(hop1.at[0], hop1.at[0], s, r, device_id={"tp": other}, device_id_type=MESH)

    def run_legs(legs):
        for _, o, axis, i in legs:
            if i:
                full(send.at[0], recv.at[LEG_ID[o, i - 1]]).wait_recv()
            to = leg_peer(me, core, o, axis)
            if i == N_LEGS[o] - 1:
                for c in last_copies(o, source(o, i), to):
                    c.start()
            else:
                k = LEG_ID[o, i]
                pltpu.make_async_remote_copy(source(o, i), hops[i].at[JOB_ID[o]], send.at[k], recv.at[k], device_id={"ep": to}, device_id_type=MESH).start()

    done_times = [max(FINISH_ALL[o] for o in DONE_ORDER[g * per:(g + 1) * per]) + LAG for g in range(n_chunk)]
    groups = group_events(done_times)

    x_copy = pltpu.make_async_copy(x_ref.at[:, mine], xh, lsem.at[0])
    own = pltpu.make_async_copy(z_ref.at[DONE_SLOT[SELF]].at[:, mine], back.at[DONE_SLOT[SELF], core], lsem.at[1])
    _, cross = last_copies(SELF, z_ref.at[DONE_SLOT[SELF]], None)
    first = [leg for leg in groups[0] if leg[3] == 0]
    run_legs(first)
    groups[0] = [leg for leg in groups[0] if leg[3] != 0]
    for c in (own, cross, x_copy):
        c.start()

    tables = ((idx_ref[...], ids), (gate_ref[...], gts))
    eye = lax.broadcasted_iota(jnp.int32, (rows, rows), 0) == lax.broadcasted_iota(jnp.int32, (rows, rows), 1)
    n_owner = idx_ref.shape[1]
    own_experts = n_par
    for g in range(n_chunk):
        lanes = []
        for o in DONE_ORDER[g * per:(g + 1) * per]:
            for p in range(n_par):
                lanes.append(own_experts * peer_at(me, p, neg(o)) + p)
        for table, rows_out in tables:
            col = jnp.concatenate([lane_column(table, e) for e in lanes], axis=0)
            rows_out[g:g + 1, :] = jnp.sum(jnp.where(eye, col, 0.0), axis=0, keepdims=True)

    def combine(g, c):
        for k in range(n_chunk):
            @pl.when(g == k)
            def _():
                run_legs(groups[k])
                if k == n_chunk - 1:
                    run_legs(groups[n_chunk])
                for o in DONE_ORDER[k * per:(k + 1) * per]:
                    j = DONE_SLOT[o]
                    if o == SELF:
                        own.wait()
                    else:
                        dummy(asend.at[j], arecv.at[j]).wait_recv()
                    dummy(bsend.at[j], brecv.at[j]).wait_recv()
        z = back[pl.ds(g * per, per)].reshape(rows, half)
        hit = lax.broadcasted_iota(jnp.int32, (n_tok, rows), 0).astype(jnp.float32) == ids[pl.ds(g, 1), :]
        left = gts[pl.ds(g, 1), :]
        total = None
        for _ in range(3):
            piece = left.astype(jnp.bfloat16)
            left = left - piece.astype(jnp.float32)
            mat = jnp.where(hit, piece.astype(jnp.float32), 0.0).astype(jnp.bfloat16)
            part = jnp.dot(mat, z, preferred_element_type=jnp.float32)
            total = part if total is None else total + part

        @pl.when(g == 0)
        def _():
            acc[...] = total

        @pl.when(g > 0)
        def _():
            acc[...] += total
        return c

    lax.fori_loop(0, n_chunk, combine, 0)
    x_copy.wait()
    n_part = osend.shape[0]
    size = n_tok // n_part

    def out_copies(b):
        at = pl.ds(pl.multiple_of(b * size, size), size)
        src, dst = obuf.at[at], out_ref.at[at, mine]
        return (pltpu.make_async_copy(src, dst, osem.at[b]),
                pltpu.make_async_remote_copy(src, dst, osend.at[b], orecv.at[b], device_id={"tp": other}, device_id_type=MESH))

    def finish(b, c):
        at = pl.ds(pl.multiple_of(b * size, size), size)
        obuf[at, :] = (xh[at, :].astype(jnp.float32) + acc[at, :]).astype(jnp.bfloat16)
        for copy in out_copies(b):
            copy.start()
        return c

    lax.fori_loop(0, n_part, finish, 0)

    def drain_out(b, c):
        for copy in out_copies(b):
            copy.wait()
        return c

    lax.fori_loop(0, n_part, drain_out, 0)
    for leg in LEGS:
        if leg[3] < N_LEGS[leg[1]] - 1:
            full(send.at[LEG_ID[leg[1], leg[3]]], recv.at[0]).wait_send()

    def drain(j, c):
        @pl.when(j != DONE_SLOT[SELF])
        def _():
            dummy(asend.at[j], arecv.at[j]).wait_send()
        dummy(bsend.at[j], brecv.at[j]).wait_send()
        return c

    lax.fori_loop(0, n_slot, drain, 0)


def solution(mesh):
    n_groups = mesh.shape["ep"]
    any_spec = pl.BlockSpec(memory_space=pl.ANY)
    vmem_spec = pl.BlockSpec(memory_space=pltpu.VMEM)
    dma = pltpu.SemaphoreType.DMA
    n_legs, n_jobs = len(LEGS), len(FINISH)
    params = pltpu.CompilerParams(has_side_effects=True, vmem_limit_bytes=VMEM_LIMIT)

    def local_layer(x_local, logit_local, w_up, w_down):
        n_tok, d_model = x_local.shape
        n_experts = logit_local.shape[1]
        own_experts, _, hid = w_up.shape
        capacity = CAP_FACTOR * n_tok * n_groups // n_experts
        cand = 2 * capacity // n_groups
        half = d_model // 2
        block = lambda n: pltpu.VMEM((n, cand, d_model), jnp.bfloat16)

        small = jax.ShapeDtypeStruct((cand, n_experts), jnp.float32)
        val, idx, gate = pl.pallas_call(
            functools.partial(route_kernel, cand),
            out_shape=(small,) * 3,
            scratch_shapes=[pltpu.VMEM((n_tok, n_experts), jnp.float32), pltpu.VMEM((n_tok, n_experts), jnp.float32)],
        )(logit_local)
        val_send = jnp.pad(val.T, ((0, 0), (0, 128 - cand))).reshape(n_experts, 1, 128)

        z = pl.pallas_call(
            functools.partial(expert_kernel, capacity),
            out_shape=jax.ShapeDtypeStruct((n_groups, cand, d_model), jnp.bfloat16),
            in_specs=[vmem_spec, vmem_spec, any_spec, any_spec, any_spec],
            out_specs=any_spec,
            scratch_shapes=[
                pltpu.VMEM((n_groups * cand, 1), jnp.float32), block(n_groups), block(n_jobs), block(n_jobs), block(n_groups),
                pltpu.VMEM((n_groups, 1, 128), jnp.float32),
                pltpu.VMEM((2, d_model, hid), jnp.bfloat16), pltpu.VMEM((2, hid, d_model), jnp.bfloat16),
                pltpu.VMEM((2, 8, cand, d_model), jnp.bfloat16),
                dma((n_legs,)), dma((n_legs,)), dma((n_jobs,)), dma((n_jobs,)), dma((2,)), dma((2,)), dma((3,)), dma((2,)),
            ],
            compiler_params=params,
        )(idx, x_local, val_send, w_up, w_down)

        return pl.pallas_call(
            combine_kernel,
            out_shape=jax.ShapeDtypeStruct((n_tok, d_model), jnp.bfloat16),
            in_specs=[vmem_spec, vmem_spec, any_spec, any_spec],
            out_specs=any_spec,
            scratch_shapes=[
                pltpu.VMEM((n_groups // 4, 8 * cand), jnp.float32), pltpu.VMEM((n_groups // 4, 8 * cand), jnp.float32),
                block(n_jobs), block(n_jobs),
                pltpu.VMEM((n_groups, own_experts, cand, half), jnp.bfloat16),
                pltpu.VMEM((n_tok, half), jnp.float32), pltpu.VMEM((n_tok, half), jnp.bfloat16), pltpu.VMEM((n_tok, half), jnp.bfloat16),
                dma((n_legs,)), dma((n_legs,)), dma((n_groups,)), dma((n_groups,)), dma((n_groups,)), dma((n_groups,)),
                dma((2,)), dma((4,)), dma((4,)), dma((4,)),
            ],
            compiler_params=params,
        )(idx, gate, x_local, z)

    token_spec = P(("dp", "ep"), None)
    return jax.shard_map(local_layer, mesh=mesh, in_specs=(token_spec, token_spec, P("ep", None, "tp"), P("ep", "tp", None)), out_specs=token_spec, check_vma=False)
```

```python
import functools

import jax
import jax.numpy as jnp
from jax import lax
from jax.experimental import pallas as pl
from jax.experimental.pallas import tpu as pltpu
from jax.sharding import PartitionSpec as P

CAP_FACTOR = 2
MESH = pl.DeviceIdType.MESH
SIDE = 4
LAG = 12.0
EARLY = 10.0
EARLY_HOP = 6.0
AHEAD = 2.0
DONE_LAG = 5.0
EXPERT_COST = 3.0
PICK_PER, EXPERT_PER, COMBINE_PER = 8, 8, 4
VMEM_LIMIT = 67043328
SELF = (0, 0, 0)


def neg(off):
    return tuple((-v) % SIDE for v in off)


def plan(priority, lag, release, begin):
    jobs = [(p // 16, p // 4 % 4, p % 4) for p in priority]
    dur = {1: 1.0, 3: 1.0, 2: 2.0}
    rem = {o: {d for d in range(3) if o[d]} for o in jobs}
    ready = dict(release)
    count = {o: 0 for o in jobs}
    free = list(begin)
    legs = []
    while any(rem.values()):
        d = min((d for d in range(3) if any(d in rem[o] for o in jobs)), key=lambda d: free[d])
        cand = [o for o in jobs if d in rem[o]]
        avail = [o for o in cand if ready[o] <= free[d] + 1e-9]
        if not avail:
            free[d] = min(ready[o] for o in cand)
            continue
        o = avail[0]
        rem[o].discard(d)
        legs.append((free[d], o, d, count[o]))
        count[o] += 1
        free[d] += dur[o[d]]
        ready[o] = free[d] + lag
    return sorted(legs), {o: ready[o] - lag for o in jobs}, free


OUT_PRIORITY = (3, 39, 31, 61, 40, 26, 34, 58, 44, 51, 33, 12, 27, 62, 41, 4, 22, 17, 21, 11, 52, 23, 45, 60, 7, 49, 18, 36, 35, 13, 57, 32, 43, 15, 47, 59, 8, 55, 5, 46, 10, 24, 54, 50, 20, 9, 38, 29, 2, 63, 28, 1, 14, 56, 53, 42, 48, 37, 6, 30, 25, 19, 16)
BACK_PRIORITY = (7, 37, 39, 47, 6, 58, 28, 13, 23, 24, 57, 11, 4, 22, 1, 43, 27, 32, 41, 2, 63, 52, 62, 59, 61, 60, 17, 3, 38, 36, 26, 16, 19, 34, 42, 49, 21, 53, 29, 14, 31, 46, 30, 54, 20, 35, 33, 12, 45, 51, 10, 25, 8, 9, 48, 56, 15, 18, 50, 5, 40, 44, 55)
OFFSETS = [(a, b, c) for a in range(SIDE) for b in range(SIDE) for c in range(SIDE) if a or b or c]
N_LEGS = {o: sum(1 for v in o if v) for o in OFFSETS}
JOB_ID = {o: j for j, o in enumerate(sorted(OFFSETS, key=lambda o: (-N_LEGS[o], o)))}
N_HOP = [sum(1 for o in OFFSETS if N_LEGS[o] > i) for i in (1, 2)]

OUT_LEGS, OUT_DONE, AXIS_FREE = plan(OUT_PRIORITY, LAG, {o: 0.0 for o in OFFSETS}, (0.0, 0.0, 0.0))
START = {o: t for t, o, _, i in OUT_LEGS if i == 0}
SEND_ORDER = sorted(OFFSETS, key=lambda o: (START[o], o)) + [SELF]
DONE_ORDER = [SELF] + sorted(OFFSETS, key=lambda o: (OUT_DONE[o], o))
SEND_SLOT = {o: p for p, o in enumerate(SEND_ORDER)}
DONE_SLOT = {o: r for r, o in enumerate(DONE_ORDER)}
LEG_ID = {(o, i): k for k, (_, o, _, i) in enumerate(OUT_LEGS)}
N_CHUNK = len(DONE_ORDER) // EXPERT_PER
N_BACK = len(DONE_ORDER) // COMBINE_PER


def chunks(order, per):
    return [order[g:g + per] for g in range(0, len(order), per)]


PICK_TIMES = [min(START[o] for o in c if o != SELF) - EARLY - AHEAD for c in chunks(SEND_ORDER, PICK_PER)]
EXPERT_TIMES = []
for group in chunks(DONE_ORDER, EXPERT_PER):
    at = max(OUT_DONE.get(o, 0.0) for o in group) + DONE_LAG
    EXPERT_TIMES.append(max(at, EXPERT_TIMES[-1] + EXPERT_COST) if EXPERT_TIMES else at)
PICK_TIMES = [min(t, EXPERT_TIMES[0] - 1.0 - 0.01 * (N_CHUNK - g)) for g, t in enumerate(PICK_TIMES)]
RELEASE = {o: EXPERT_TIMES[DONE_SLOT[neg(o)] // EXPERT_PER] + EXPERT_COST + EARLY for o in OFFSETS}
BACK_LEGS, BACK_DONE, _ = plan(BACK_PRIORITY, LAG, RELEASE, AXIS_FREE)
BACK_ID = {(o, i): k for k, (_, o, _, i) in enumerate(BACK_LEGS)}
BACK_ORDER = [SELF] + sorted(OFFSETS, key=lambda o: (BACK_DONE[o], o))
BACK_SLOT = {o: r for r, o in enumerate(BACK_ORDER)}
BACK_TIMES = [max(BACK_DONE.get(o, 0.0) for o in c) + DONE_LAG for c in chunks(BACK_ORDER, COMBINE_PER)]
BACK_TIMES = [max(t, EXPERT_TIMES[-1] + EXPERT_COST) for t in BACK_TIMES]


def group_events():
    rest = [(t - (EARLY_HOP if i else EARLY), kind, (o, axis, i)) for kind, legs in ((0, OUT_LEGS), (1, BACK_LEGS)) for t, o, axis, i in legs]
    rest.sort()
    groups = []
    for t in PICK_TIMES + EXPERT_TIMES + BACK_TIMES:
        groups.append([e[1:] for e in rest if e[0] < t])
        rest = [e for e in rest if e[0] >= t]
    return groups + [[e[1:] for e in rest]]


GROUPS = group_events()


def axis_peers(me, sign):
    z = lax.div(me, SIDE * SIDE)
    y = lax.rem(lax.div(me, SIDE), SIDE)
    x = lax.rem(me, SIDE)
    return [[lax.rem(p + v + sign * (2 * SIDE - 2 * v), SIDE) * scale for v in range(SIDE)] for p, scale in ((z, SIDE * SIDE), (y, SIDE), (x, 1))]


def peer_at(table, off):
    return table[0][off[0]] + table[1][off[1]] + table[2][off[2]]


def leg_peer(table, off, axis):
    return peer_at(table, tuple(v if q == axis else 0 for q, v in enumerate(off)))


def lane_column(table, lane):
    lanes = lax.broadcasted_iota(jnp.int32, table.shape, 1)
    return jnp.sum(jnp.where(lanes == lane, table, 0.0), axis=1, keepdims=True)


def route_kernel(n_cand, logit_ref, val_ref, idx_ref, gate_ref, work, soft):
    n_tok, lanes = logit_ref.shape
    step = 64
    best = jnp.full((8, lanes), -jnp.inf, jnp.float32)
    for lo in range(0, n_tok, step):
        v = logit_ref[lo:lo + step, :]
        e = jnp.exp(v - jnp.max(v, axis=1, keepdims=True))
        soft[lo:lo + step, :] = e / jnp.sum(e, axis=1, keepdims=True)
        work[lo:lo + step, :] = v
        best = jnp.maximum(best, jnp.max(v.reshape(step // 8, 8, lanes), axis=0))
    row = lax.broadcasted_iota(jnp.int32, (step, lanes), 0).astype(jnp.float32)

    def body(k, best):
        top = jnp.max(best, axis=0, keepdims=True)
        nxt = jnp.full((8, lanes), -jnp.inf, jnp.float32)
        pos = jnp.zeros((8, lanes), jnp.float32)
        gat = jnp.zeros((8, lanes), jnp.float32)
        for lo in range(0, n_tok, step):
            v = work[lo:lo + step, :]
            hit = v == top
            v = jnp.where(hit, -jnp.inf, v)
            work[lo:lo + step, :] = v
            nxt = jnp.maximum(nxt, jnp.max(v.reshape(step // 8, 8, lanes), axis=0))
            pos = pos + jnp.sum(jnp.where(hit, row + float(lo), 0.0).reshape(step // 8, 8, lanes), axis=0)
            gat = gat + jnp.sum(jnp.where(hit, soft[lo:lo + step, :], 0.0).reshape(step // 8, 8, lanes), axis=0)
        val_ref[pl.ds(k, 1), :] = top
        idx_ref[pl.ds(k, 1), :] = jnp.sum(pos, axis=0, keepdims=True)
        gate_ref[pl.ds(k, 1), :] = jnp.sum(gat, axis=0, keepdims=True)
        return nxt

    lax.fori_loop(0, n_cand, body, best)


def layer_kernel(capacity, idx_ref, gate_ref, x_ref, val_ref, wu_ref, wd_ref, out_ref, back1, back2,
                 cols, ids, gts, outbox, hop1, hop2, inbox, rval, wu, wd, back, acc, obuf,
                 send, recv, vsend, vrecv, wsend, wrecv, lsem, rsend, rrecv, asend, arecv, bsend, brecv, osend, orecv, osem):
    me, core = lax.axis_index("ep"), lax.axis_index("tp")
    other = 1 - core
    table = axis_peers(me, core)
    tables = [axis_peers(me, p) for p in range(back.shape[1])]
    n_slot, cand, d_model = outbox.shape
    n_par, half = back.shape[1], back.shape[3]
    n_tok, lanes = x_ref.shape[0], val_ref.shape[2]
    own_experts = wu_ref.shape[0]
    rows = EXPERT_PER * cand
    mine = pl.ds(pl.multiple_of(core * half, half), half)
    theirs = pl.ds(pl.multiple_of(other * half, half), half)
    hops, back_hops = (hop1, hop2), (back1, back2)

    weights = []
    for i, (src, dst) in enumerate(((wu_ref, wu), (wd_ref, wd))):
        weights.append(pltpu.make_async_copy(src.at[core], dst.at[0], lsem.at[i]))
        weights.append(pltpu.make_async_remote_copy(src.at[other], dst.at[1], wsend.at[i], wrecv.at[i], device_id={"tp": other}, device_id_type=MESH))
    own_val = pltpu.make_async_copy(val_ref.at[own_experts * me + core], rval.at[DONE_SLOT[SELF]], lsem.at[2])

    def val_copy(o):
        to = peer_at(table, o)
        j = JOB_ID[o]
        return pltpu.make_async_remote_copy(val_ref.at[own_experts * to + core], rval.at[DONE_SLOT[o]], vsend.at[j], vrecv.at[j], device_id={"ep": to}, device_id_type=MESH)

    def whole(s, r):
        return pltpu.make_async_remote_copy(inbox.at[0], inbox.at[0], s, r, device_id={"tp": other}, device_id_type=MESH)

    def part(s, r):
        return pltpu.make_async_remote_copy(back.at[0, 0], back.at[0, 0], s, r, device_id={"tp": other}, device_id_type=MESH)

    def out_leg(o, axis, i):
        if i:
            whole(send.at[0], recv.at[LEG_ID[o, i - 1]]).wait_recv()
        src = hops[i - 1].at[JOB_ID[o]] if i else outbox.at[SEND_SLOT[o]]
        dst = inbox.at[DONE_SLOT[o]] if i == N_LEGS[o] - 1 else hops[i].at[JOB_ID[o]]
        k = LEG_ID[o, i]
        pltpu.make_async_remote_copy(src, dst, send.at[k], recv.at[k], device_id={"ep": leg_peer(table, o, axis)}, device_id_type=MESH).start()

    def split_copy(o, src, h, to):
        cols_of, (s, r) = ((mine, (asend, arecv)), (theirs, (bsend, brecv)))[h]
        j = BACK_SLOT[o]
        there = {} if to is None else {"ep": to}
        if h:
            there["tp"] = other
        return pltpu.make_async_remote_copy(src.at[:, cols_of], back.at[j, core], s.at[j], r.at[j], device_id=there, device_id_type=MESH)

    def back_leg(o, axis, i):
        if i:
            whole(rsend.at[0], rrecv.at[BACK_ID[o, i - 1]]).wait_recv()
        src = back_hops[i - 1].at[JOB_ID[o]] if i else inbox.at[DONE_SLOT[neg(o)]]
        to = leg_peer(table, o, axis)
        if i == N_LEGS[o] - 1:
            for h in range(2):
                split_copy(o, src, h, to).start()
        else:
            k = BACK_ID[o, i]
            pltpu.make_async_remote_copy(src, back_hops[i].at[JOB_ID[o]], rsend.at[k], rrecv.at[k], device_id={"ep": to}, device_id_type=MESH).start()

    def run_legs(group):
        for kind, leg in group:
            (back_leg if kind else out_leg)(*leg)

    idx = idx_ref[...]

    def set_columns(p):
        cols[p * cand:(p + 1) * cand, :] = lane_column(idx, own_experts * peer_at(table, SEND_ORDER[p]) + core)

    def set_rows(g):
        at = []
        for o in BACK_ORDER[g * COMBINE_PER:(g + 1) * COMBINE_PER]:
            for p in range(n_par):
                at.append(own_experts * peer_at(tables[p], neg(o)) + p)
        n = len(at) * cand
        eye = lax.broadcasted_iota(jnp.int32, (n, n), 0) == lax.broadcasted_iota(jnp.int32, (n, n), 1)
        for source, dst in ((idx, ids), (gate_ref[...], gts)):
            col = jnp.concatenate([lane_column(source, e) for e in at], axis=0)
            dst[g:g + 1, :] = jnp.sum(jnp.where(eye, col, 0.0), axis=0, keepdims=True)

    for p in range(PICK_PER):
        set_columns(p)

    def pick(g, c):
        for k in range(N_CHUNK):
            @pl.when(g == k)
            def _():
                run_legs(GROUPS[k])
        at = pl.multiple_of(g * rows, rows)
        onehot = (lax.broadcasted_iota(jnp.int32, (rows, n_tok), 1).astype(jnp.float32) == cols[pl.ds(at, rows), :]).astype(jnp.bfloat16)
        got = jnp.dot(onehot, x_ref[...], preferred_element_type=jnp.float32).astype(jnp.bfloat16)
        outbox[pl.ds(g * PICK_PER, PICK_PER)] = got.reshape(PICK_PER, cand, d_model)
        for k in range(N_CHUNK):
            @pl.when(g == k)
            def _():
                if k == 0:
                    for w in weights + [own_val]:
                        w.start()
                    for o in OFFSETS:
                        val_copy(o).start()
                if k < N_CHUNK - 1:
                    for p in range((k + 1) * PICK_PER, (k + 2) * PICK_PER):
                        set_columns(p)
                for b in range(k * N_BACK // N_CHUNK, (k + 1) * N_BACK // N_CHUNK):
                    set_rows(b)
        return c

    lax.fori_loop(0, N_CHUNK, pick, 0)
    inbox[DONE_SLOT[SELF]] = outbox[SEND_SLOT[SELF]]

    def expert(g, c):
        for k in range(N_CHUNK):
            @pl.when(g == k)
            def _():
                run_legs(GROUPS[N_CHUNK + k])
                if k == 0:
                    for o in OFFSETS:
                        val_copy(o).wait_recv()
                    for w in weights + [own_val]:
                        w.wait()
                for o in DONE_ORDER[k * EXPERT_PER:(k + 1) * EXPERT_PER]:
                    if o != SELF:
                        whole(send.at[0], recv.at[LEG_ID[o, N_LEGS[o] - 1]]).wait_recv()
        eye = lax.broadcasted_iota(jnp.int32, (cand, lanes), 0) == lax.broadcasted_iota(jnp.int32, (cand, lanes), 1)
        value = jnp.concatenate([jnp.sum(jnp.where(eye, rval[g * EXPERT_PER + i], 0.0), axis=1, keepdims=True) for i in range(EXPERT_PER)], axis=0)
        real = lax.broadcasted_iota(jnp.int32, (1, lanes), 1) < cand

        def count(j, total):
            return total + (jnp.where(real, rval[j], -jnp.inf) > value).astype(jnp.float32)

        above = lax.fori_loop(0, n_slot, count, jnp.zeros((rows, lanes), jnp.float32), unroll=8)
        keep = jnp.sum(above, axis=1, keepdims=True) < float(capacity)
        here = pl.ds(g * EXPERT_PER, EXPERT_PER)
        x = inbox[here].reshape(rows, d_model)
        z = None
        for h in range(2):
            pre = jnp.dot(x, wu[h], preferred_element_type=jnp.float32)
            hid = jax.nn.gelu(pre, approximate=True).astype(jnp.bfloat16)
            term = jnp.dot(hid, wd[h], preferred_element_type=jnp.float32)
            z = term if z is None else z + term
        inbox[here] = jnp.where(keep, z, 0.0).astype(jnp.bfloat16).reshape(EXPERT_PER, cand, d_model)
        return c

    lax.fori_loop(0, N_CHUNK, expert, 0)

    def combine(g, c):
        for k in range(N_BACK):
            @pl.when(g == k)
            def _():
                run_legs(GROUPS[2 * N_CHUNK + k])
                if k == 0:
                    for p in range(n_par):
                        @pl.when(core == p)
                        def _():
                            back[BACK_SLOT[SELF], p] = inbox[DONE_SLOT[SELF], :, p * half:(p + 1) * half]
                    split_copy(SELF, inbox.at[DONE_SLOT[SELF]], 1, None).start()
                if k == N_BACK - 1:
                    run_legs(GROUPS[2 * N_CHUNK + N_BACK])
                for o in BACK_ORDER[k * COMBINE_PER:(k + 1) * COMBINE_PER]:
                    j = BACK_SLOT[o]
                    if o != SELF:
                        part(asend.at[j], arecv.at[j]).wait_recv()
                    part(bsend.at[j], brecv.at[j]).wait_recv()
        n = ids.shape[1]
        z = back[pl.ds(g * COMBINE_PER, COMBINE_PER)].reshape(n, half)
        hit = lax.broadcasted_iota(jnp.int32, (n_tok, n), 0).astype(jnp.float32) == ids[pl.ds(g, 1), :]
        left = gts[pl.ds(g, 1), :]
        total = None
        for _ in range(3):
            piece = left.astype(jnp.bfloat16)
            left = left - piece.astype(jnp.float32)
            mat = jnp.where(hit, piece.astype(jnp.float32), 0.0).astype(jnp.bfloat16)
            term = jnp.dot(mat, z, preferred_element_type=jnp.float32)
            total = term if total is None else total + term

        @pl.when(g == 0)
        def _():
            acc[...] = total

        @pl.when(g > 0)
        def _():
            acc[...] += total
        return c

    lax.fori_loop(0, N_BACK, combine, 0)
    n_part = osend.shape[0]
    size = n_tok // n_part

    def out_copies(b):
        at = pl.ds(pl.multiple_of(b * size, size), size)
        src, dst = obuf.at[at], out_ref.at[at, mine]
        return (pltpu.make_async_copy(src, dst, osem.at[b]),
                pltpu.make_async_remote_copy(src, dst, osend.at[b], orecv.at[b], device_id={"tp": other}, device_id_type=MESH))

    def finish(b, c):
        at = pl.ds(pl.multiple_of(b * size, size), size)
        for p in range(n_par):
            @pl.when(core == p)
            def _():
                obuf[at, :] = (x_ref[at, p * half:(p + 1) * half].astype(jnp.float32) + acc[at, :]).astype(jnp.bfloat16)
        for copy in out_copies(b):
            copy.start()
        return c

    lax.fori_loop(0, n_part, finish, 0)

    def drain_legs(k, c):
        whole(send.at[k], recv.at[0]).wait_send()
        return c

    lax.fori_loop(0, len(OUT_LEGS), drain_legs, 0)

    def drain_vals(j, c):
        pltpu.make_async_remote_copy(rval.at[0], rval.at[0], vsend.at[j], vrecv.at[0], device_id={"tp": other}, device_id_type=MESH).wait_send()
        return c

    lax.fori_loop(0, len(OFFSETS), drain_vals, 0)
    for _, o, _, i in BACK_LEGS:
        if i < N_LEGS[o] - 1:
            whole(rsend.at[BACK_ID[o, i]], rrecv.at[0]).wait_send()

    def drain_back(j, c):
        @pl.when(j != BACK_SLOT[SELF])
        def _():
            part(asend.at[j], arecv.at[j]).wait_send()
        part(bsend.at[j], brecv.at[j]).wait_send()
        return c

    lax.fori_loop(0, n_slot, drain_back, 0)

    def drain_out(b, c):
        for copy in out_copies(b):
            copy.wait()
        return c

    lax.fori_loop(0, n_part, drain_out, 0)


def solution(mesh):
    n_groups = mesh.shape["ep"]
    any_spec = pl.BlockSpec(memory_space=pl.ANY)
    vmem_spec = pl.BlockSpec(memory_space=pltpu.VMEM)
    dma = pltpu.SemaphoreType.DMA
    n_legs, n_jobs = len(OUT_LEGS), len(OFFSETS)

    def local_layer(x_local, logit_local, w_up, w_down):
        n_tok, d_model = x_local.shape
        n_experts = logit_local.shape[1]
        own_experts, _, hid = w_up.shape
        capacity = CAP_FACTOR * n_tok * n_groups // n_experts
        cand = 2 * capacity // n_groups
        half = d_model // 2
        n_back_rows = COMBINE_PER * own_experts * cand
        block = lambda n: pltpu.VMEM((n, cand, d_model), jnp.bfloat16)

        small = jax.ShapeDtypeStruct((cand, n_experts), jnp.float32)
        val, idx, gate = pl.pallas_call(
            functools.partial(route_kernel, cand),
            out_shape=(small,) * 3,
            scratch_shapes=[pltpu.VMEM((n_tok, n_experts), jnp.float32), pltpu.VMEM((n_tok, n_experts), jnp.float32)],
        )(logit_local)
        val_send = jnp.pad(val.T, ((0, 0), (0, 128 - cand))).reshape(n_experts, 1, 128)

        out, _, _ = pl.pallas_call(
            functools.partial(layer_kernel, capacity),
            out_shape=(
                jax.ShapeDtypeStruct((n_tok, d_model), jnp.bfloat16),
                jax.ShapeDtypeStruct((N_HOP[0], cand, d_model), jnp.bfloat16),
                jax.ShapeDtypeStruct((N_HOP[1], cand, d_model), jnp.bfloat16),
            ),
            in_specs=[vmem_spec, vmem_spec, vmem_spec, any_spec, any_spec, any_spec],
            out_specs=(any_spec,) * 3,
            scratch_shapes=[
                pltpu.VMEM((n_groups * cand, 1), jnp.float32),
                pltpu.VMEM((N_BACK, n_back_rows), jnp.float32), pltpu.VMEM((N_BACK, n_back_rows), jnp.float32),
                block(n_groups), block(N_HOP[0]), block(N_HOP[1]), block(n_groups),
                pltpu.VMEM((n_groups, 1, 128), jnp.float32),
                pltpu.VMEM((2, d_model, hid), jnp.bfloat16), pltpu.VMEM((2, hid, d_model), jnp.bfloat16),
                pltpu.VMEM((n_groups, own_experts, cand, half), jnp.bfloat16),
                pltpu.VMEM((n_tok, half), jnp.float32), pltpu.VMEM((n_tok, half), jnp.bfloat16),
                dma((n_legs,)), dma((n_legs,)), dma((n_jobs,)), dma((n_jobs,)), dma((2,)), dma((2,)), dma((3,)),
                dma((n_legs,)), dma((n_legs,)), dma((n_groups,)), dma((n_groups,)), dma((n_groups,)), dma((n_groups,)),
                dma((4,)), dma((4,)), dma((4,)),
            ],
            compiler_params=pltpu.CompilerParams(has_side_effects=True, vmem_limit_bytes=VMEM_LIMIT),
        )(idx, gate, x_local, val_send, w_up, w_down)
        return out

    token_spec = P(("dp", "ep"), None)
    return jax.shard_map(local_layer, mesh=mesh, in_specs=(token_spec, token_spec, P("ep", None, "tp"), P("ep", "tp", None)), out_specs=token_spec, check_vma=False)
```

```python
import functools

import jax
import jax.numpy as jnp
from jax import lax
from jax.experimental import pallas as pl
from jax.experimental.pallas import tpu as pltpu
from jax.sharding import PartitionSpec as P

CAP_FACTOR = 2
MESH = pl.DeviceIdType.MESH
SIDE = 4
LAG = 12.0
EARLY = 10.0
EARLY_HOP = 6.0
AHEAD = 2.0
DONE_LAG = 5.0
EXPERT_COST = 3.0
PICK_PER, EXPERT_PER, COMBINE_PER = 8, 8, 4
VMEM_LIMIT = 67043328
SELF = (0, 0, 0)


def neg(off):
    return tuple((-v) % SIDE for v in off)


def plan(priority, lag, release, begin):
    jobs = [(p // 16, p // 4 % 4, p % 4) for p in priority]
    dur = {1: 1.0, 3: 1.0, 2: 2.0}
    rem = {o: {d for d in range(3) if o[d]} for o in jobs}
    ready = dict(release)
    count = {o: 0 for o in jobs}
    free = list(begin)
    legs = []
    while any(rem.values()):
        d = min((d for d in range(3) if any(d in rem[o] for o in jobs)), key=lambda d: free[d])
        cand = [o for o in jobs if d in rem[o]]
        avail = [o for o in cand if ready[o] <= free[d] + 1e-9]
        if not avail:
            free[d] = min(ready[o] for o in cand)
            continue
        o = avail[0]
        rem[o].discard(d)
        legs.append((free[d], o, d, count[o]))
        count[o] += 1
        free[d] += dur[o[d]]
        ready[o] = free[d] + lag
    return sorted(legs), {o: ready[o] - lag for o in jobs}, free


OUT_PRIORITY = (3, 39, 31, 61, 40, 26, 34, 58, 44, 51, 33, 12, 27, 62, 41, 4, 22, 17, 21, 11, 52, 23, 45, 60, 7, 49, 18, 36, 35, 13, 57, 32, 43, 15, 47, 59, 8, 55, 5, 46, 10, 24, 54, 50, 20, 9, 38, 29, 2, 63, 28, 1, 14, 56, 53, 42, 48, 37, 6, 30, 25, 19, 16)
BACK_PRIORITY = (7, 37, 39, 47, 6, 58, 28, 13, 23, 24, 57, 11, 4, 22, 1, 43, 27, 32, 41, 2, 63, 52, 62, 59, 61, 60, 17, 3, 38, 36, 26, 16, 19, 34, 42, 49, 21, 53, 29, 14, 31, 46, 30, 54, 20, 35, 33, 12, 45, 51, 10, 25, 8, 9, 48, 56, 15, 18, 50, 5, 40, 44, 55)
OFFSETS = [(a, b, c) for a in range(SIDE) for b in range(SIDE) for c in range(SIDE) if a or b or c]
N_LEGS = {o: sum(1 for v in o if v) for o in OFFSETS}
JOB_ID = {o: j for j, o in enumerate(sorted(OFFSETS, key=lambda o: (-N_LEGS[o], o)))}
N_HOP = [sum(1 for o in OFFSETS if N_LEGS[o] > i) for i in (1, 2)]

OUT_LEGS, OUT_DONE, AXIS_FREE = plan(OUT_PRIORITY, LAG, {o: 0.0 for o in OFFSETS}, (0.0, 0.0, 0.0))
START = {o: t for t, o, _, i in OUT_LEGS if i == 0}
SEND_ORDER = sorted(OFFSETS, key=lambda o: (START[o], o)) + [SELF]
DONE_ORDER = [SELF] + sorted(OFFSETS, key=lambda o: (OUT_DONE[o], o))
SEND_SLOT = {o: p for p, o in enumerate(SEND_ORDER)}
DONE_SLOT = {o: r for r, o in enumerate(DONE_ORDER)}
LEG_ID = {(o, i): k for k, (_, o, _, i) in enumerate(OUT_LEGS)}
N_CHUNK = len(DONE_ORDER) // EXPERT_PER
N_BACK = len(DONE_ORDER) // COMBINE_PER


def chunks(order, per):
    return [order[g:g + per] for g in range(0, len(order), per)]


PICK_TIMES = [min(START[o] for o in c if o != SELF) - EARLY - AHEAD for c in chunks(SEND_ORDER, PICK_PER)]
EXPERT_TIMES = []
for group in chunks(DONE_ORDER, EXPERT_PER):
    at = max(OUT_DONE.get(o, 0.0) for o in group) + DONE_LAG
    EXPERT_TIMES.append(max(at, EXPERT_TIMES[-1] + EXPERT_COST) if EXPERT_TIMES else at)
PICK_TIMES = [min(t, EXPERT_TIMES[0] - 1.0 - 0.01 * (N_CHUNK - g)) for g, t in enumerate(PICK_TIMES)]
RELEASE = {o: EXPERT_TIMES[DONE_SLOT[neg(o)] // EXPERT_PER] + EXPERT_COST + EARLY for o in OFFSETS}
BACK_LEGS, BACK_DONE, _ = plan(BACK_PRIORITY, LAG, RELEASE, AXIS_FREE)
BACK_ID = {(o, i): k for k, (_, o, _, i) in enumerate(BACK_LEGS)}
BACK_ORDER = [SELF] + sorted(OFFSETS, key=lambda o: (BACK_DONE[o], o))
BACK_SLOT = {o: r for r, o in enumerate(BACK_ORDER)}
BACK_TIMES = [max(BACK_DONE.get(o, 0.0) for o in c) + DONE_LAG for c in chunks(BACK_ORDER, COMBINE_PER)]
BACK_TIMES = [max(t, EXPERT_TIMES[-1] + EXPERT_COST) for t in BACK_TIMES]


def group_events():
    rest = [(t - (EARLY_HOP if i else EARLY), kind, (o, axis, i)) for kind, legs in ((0, OUT_LEGS), (1, BACK_LEGS)) for t, o, axis, i in legs]
    rest.sort()
    groups = []
    for t in PICK_TIMES + EXPERT_TIMES + BACK_TIMES:
        groups.append([e[1:] for e in rest if e[0] < t])
        rest = [e for e in rest if e[0] >= t]
    return groups + [[e[1:] for e in rest]]


GROUPS = group_events()


def axis_peers(me, sign):
    z = lax.div(me, SIDE * SIDE)
    y = lax.rem(lax.div(me, SIDE), SIDE)
    x = lax.rem(me, SIDE)
    return [[lax.rem(p + v + sign * (2 * SIDE - 2 * v), SIDE) * scale for v in range(SIDE)] for p, scale in ((z, SIDE * SIDE), (y, SIDE), (x, 1))]


def peer_at(table, off):
    return table[0][off[0]] + table[1][off[1]] + table[2][off[2]]


def leg_peer(table, off, axis):
    return peer_at(table, tuple(v if q == axis else 0 for q, v in enumerate(off)))


def lane_column(table, lane):
    lanes = lax.broadcasted_iota(jnp.int32, table.shape, 1)
    return jnp.sum(jnp.where(lanes == lane, table, 0.0), axis=1, keepdims=True)


def route(n_cand, logit_ref, val_ref, idx_ref, gate_ref, work, soft):
    n_tok, lanes = logit_ref.shape
    step = 64
    best = jnp.full((8, lanes), -jnp.inf, jnp.float32)
    for lo in range(0, n_tok, step):
        v = logit_ref[lo:lo + step, :]
        e = jnp.exp(v - jnp.max(v, axis=1, keepdims=True))
        soft[lo:lo + step, :] = e / jnp.sum(e, axis=1, keepdims=True)
        work[lo:lo + step, :] = v
        best = jnp.maximum(best, jnp.max(v.reshape(step // 8, 8, lanes), axis=0))
    row = lax.broadcasted_iota(jnp.int32, (step, lanes), 0).astype(jnp.float32)

    def body(k, best):
        top = jnp.max(best, axis=0, keepdims=True)
        nxt = jnp.full((8, lanes), -jnp.inf, jnp.float32)
        pos = jnp.zeros((8, lanes), jnp.float32)
        gat = jnp.zeros((8, lanes), jnp.float32)
        for lo in range(0, n_tok, step):
            v = work[lo:lo + step, :]
            hit = v == top
            v = jnp.where(hit, -jnp.inf, v)
            work[lo:lo + step, :] = v
            nxt = jnp.maximum(nxt, jnp.max(v.reshape(step // 8, 8, lanes), axis=0))
            pos = pos + jnp.sum(jnp.where(hit, row + float(lo), 0.0).reshape(step // 8, 8, lanes), axis=0)
            gat = gat + jnp.sum(jnp.where(hit, soft[lo:lo + step, :], 0.0).reshape(step // 8, 8, lanes), axis=0)
        val_ref[pl.ds(k, 1), :] = top
        idx_ref[pl.ds(k, 1), :] = jnp.sum(pos, axis=0, keepdims=True)
        gate_ref[pl.ds(k, 1), :] = jnp.sum(gat, axis=0, keepdims=True)
        return nxt

    lax.fori_loop(0, n_cand, body, best)


def layer_kernel(capacity, logit_ref, x_hbm, wu_ref, wd_ref, out_ref, back1, back2,
                 x_ref, val_tab, idx_tab, gate_tab, work, soft, vals, cols, ids, gts, outbox, hop1, hop2, inbox, rval, wu, wd, back, acc, obuf,
                 send, recv, vsend, vrecv, wsend, wrecv, lsem, rsend, rrecv, asend, arecv, bsend, brecv, osend, orecv, osem, xsem):
    me, core = lax.axis_index("ep"), lax.axis_index("tp")
    other = 1 - core
    table = axis_peers(me, core)
    tables = [axis_peers(me, p) for p in range(back.shape[1])]
    n_slot, cand, d_model = outbox.shape
    n_par, half = back.shape[1], back.shape[3]
    n_tok, lanes = x_ref.shape[0], vals.shape[2]
    own_experts = wu_ref.shape[0]
    rows = EXPERT_PER * cand
    mine = pl.ds(pl.multiple_of(core * half, half), half)
    theirs = pl.ds(pl.multiple_of(other * half, half), half)
    hops, back_hops = (hop1, hop2), (back1, back2)

    barrier = pltpu.get_barrier_semaphore()
    greet = [{"ep": peer_at(table, o)} for o in OFFSETS]
    greet += [{"ep": peer_at(table, o), "tp": other} for o in OFFSETS if N_LEGS[o] == 1] + [{"tp": other}]
    for there in greet:
        pl.semaphore_signal(barrier, inc=1, device_id=there, device_id_type=MESH)
    x_copy = pltpu.make_async_copy(x_hbm, x_ref, xsem)
    x_copy.start()
    route(cand, logit_ref, val_tab, idx_tab, gate_tab, work, soft)

    weights = []
    for i, (src, dst) in enumerate(((wu_ref, wu), (wd_ref, wd))):
        weights.append(pltpu.make_async_copy(src.at[core], dst.at[0], lsem.at[i]))
        weights.append(pltpu.make_async_remote_copy(src.at[other], dst.at[1], wsend.at[i], wrecv.at[i], device_id={"tp": other}, device_id_type=MESH))
    def val_copy(o):
        to = peer_at(table, o)
        j = JOB_ID[o]
        return pltpu.make_async_remote_copy(vals.at[SEND_SLOT[o]], rval.at[DONE_SLOT[o]], vsend.at[j], vrecv.at[j], device_id={"ep": to}, device_id_type=MESH)

    def whole(s, r):
        return pltpu.make_async_remote_copy(inbox.at[0], inbox.at[0], s, r, device_id={"tp": other}, device_id_type=MESH)

    def part(s, r):
        return pltpu.make_async_remote_copy(back.at[0, 0], back.at[0, 0], s, r, device_id={"tp": other}, device_id_type=MESH)

    def out_leg(o, axis, i):
        if i:
            whole(send.at[0], recv.at[LEG_ID[o, i - 1]]).wait_recv()
        src = hops[i - 1].at[JOB_ID[o]] if i else outbox.at[SEND_SLOT[o]]
        dst = inbox.at[DONE_SLOT[o]] if i == N_LEGS[o] - 1 else hops[i].at[JOB_ID[o]]
        k = LEG_ID[o, i]
        pltpu.make_async_remote_copy(src, dst, send.at[k], recv.at[k], device_id={"ep": leg_peer(table, o, axis)}, device_id_type=MESH).start()

    def split_copy(o, src, h, to):
        cols_of, (s, r) = ((mine, (asend, arecv)), (theirs, (bsend, brecv)))[h]
        j = BACK_SLOT[o]
        there = {} if to is None else {"ep": to}
        if h:
            there["tp"] = other
        return pltpu.make_async_remote_copy(src.at[:, cols_of], back.at[j, core], s.at[j], r.at[j], device_id=there, device_id_type=MESH)

    def back_leg(o, axis, i):
        if i:
            whole(rsend.at[0], rrecv.at[BACK_ID[o, i - 1]]).wait_recv()
        src = back_hops[i - 1].at[JOB_ID[o]] if i else inbox.at[DONE_SLOT[neg(o)]]
        to = leg_peer(table, o, axis)
        if i == N_LEGS[o] - 1:
            for h in range(2):
                split_copy(o, src, h, to).start()
        else:
            k = BACK_ID[o, i]
            pltpu.make_async_remote_copy(src, back_hops[i].at[JOB_ID[o]], rsend.at[k], rrecv.at[k], device_id={"ep": to}, device_id_type=MESH).start()

    def run_legs(group):
        for kind, leg in group:
            (back_leg if kind else out_leg)(*leg)

    val, idx, gate = val_tab[...], idx_tab[...], gate_tab[...]
    diagonal = lax.broadcasted_iota(jnp.int32, (cand, lanes), 0) == lax.broadcasted_iota(jnp.int32, (cand, lanes), 1)

    def set_columns(p):
        e = own_experts * peer_at(table, SEND_ORDER[p]) + core
        cols[p * cand:(p + 1) * cand, :] = lane_column(idx, e)
        vals[p] = jnp.sum(jnp.where(diagonal, lane_column(val, e), 0.0), axis=0, keepdims=True)

    def set_rows(g):
        at = []
        for o in BACK_ORDER[g * COMBINE_PER:(g + 1) * COMBINE_PER]:
            for p in range(n_par):
                at.append(own_experts * peer_at(tables[p], neg(o)) + p)
        n = len(at) * cand
        eye = lax.broadcasted_iota(jnp.int32, (n, n), 0) == lax.broadcasted_iota(jnp.int32, (n, n), 1)
        for source, dst in ((idx, ids), (gate, gts)):
            col = jnp.concatenate([lane_column(source, e) for e in at], axis=0)
            dst[g:g + 1, :] = jnp.sum(jnp.where(eye, col, 0.0), axis=0, keepdims=True)

    for p in range(PICK_PER):
        set_columns(p)
    x_copy.wait()

    def gather(g):
        at = pl.multiple_of(g * rows, rows)
        onehot = (lax.broadcasted_iota(jnp.int32, (rows, n_tok), 1).astype(jnp.float32) == cols[pl.ds(at, rows), :]).astype(jnp.bfloat16)
        got = jnp.dot(onehot, x_ref[...], preferred_element_type=jnp.float32).astype(jnp.bfloat16)
        outbox[pl.ds(g * PICK_PER, PICK_PER)] = got.reshape(PICK_PER, cand, d_model)

    gather(0)
    pl.semaphore_wait(barrier, len(greet))

    def pick(g, c):
        for k in range(1, N_CHUNK):
            @pl.when(g == k)
            def _():
                run_legs(GROUPS[0] + GROUPS[1] if k == 1 else GROUPS[k])
                if k == 1:
                    for w in weights:
                        w.start()
                    for p in range(PICK_PER, n_slot):
                        set_columns(p)
        gather(g)
        for k in range(1, N_CHUNK):
            @pl.when(g == k)
            def _():
                if k == 1:
                    for o in OFFSETS:
                        val_copy(o).start()
                for b in range((k - 1) * N_BACK // (N_CHUNK - 1), k * N_BACK // (N_CHUNK - 1)):
                    set_rows(b)
        return c

    lax.fori_loop(1, N_CHUNK, pick, 0)
    inbox[DONE_SLOT[SELF]] = outbox[SEND_SLOT[SELF]]
    rval[DONE_SLOT[SELF]] = vals[SEND_SLOT[SELF]]

    def expert(g, c):
        for k in range(N_CHUNK):
            @pl.when(g == k)
            def _():
                run_legs(GROUPS[N_CHUNK + k])
                if k == 0:
                    for o in OFFSETS:
                        val_copy(o).wait_recv()
                    for w in weights:
                        w.wait()
                for o in DONE_ORDER[k * EXPERT_PER:(k + 1) * EXPERT_PER]:
                    if o != SELF:
                        whole(send.at[0], recv.at[LEG_ID[o, N_LEGS[o] - 1]]).wait_recv()
        eye = lax.broadcasted_iota(jnp.int32, (cand, lanes), 0) == lax.broadcasted_iota(jnp.int32, (cand, lanes), 1)
        value = jnp.concatenate([jnp.sum(jnp.where(eye, rval[g * EXPERT_PER + i], 0.0), axis=1, keepdims=True) for i in range(EXPERT_PER)], axis=0)
        real = lax.broadcasted_iota(jnp.int32, (1, lanes), 1) < cand

        def count(j, total):
            return total + (jnp.where(real, rval[j], -jnp.inf) > value).astype(jnp.float32)

        above = lax.fori_loop(0, n_slot, count, jnp.zeros((rows, lanes), jnp.float32), unroll=8)
        keep = jnp.sum(above, axis=1, keepdims=True) < float(capacity)
        here = pl.ds(g * EXPERT_PER, EXPERT_PER)
        x = inbox[here].reshape(rows, d_model)
        z = None
        for h in range(2):
            pre = jnp.dot(x, wu[h], preferred_element_type=jnp.float32)
            hid = jax.nn.gelu(pre, approximate=True).astype(jnp.bfloat16)
            term = jnp.dot(hid, wd[h], preferred_element_type=jnp.float32)
            z = term if z is None else z + term
        inbox[here] = jnp.where(keep, z, 0.0).astype(jnp.bfloat16).reshape(EXPERT_PER, cand, d_model)
        return c

    lax.fori_loop(0, N_CHUNK, expert, 0)

    def combine(g, c):
        for k in range(N_BACK):
            @pl.when(g == k)
            def _():
                run_legs(GROUPS[2 * N_CHUNK + k])
                if k == 0:
                    for p in range(n_par):
                        @pl.when(core == p)
                        def _():
                            back[BACK_SLOT[SELF], p] = inbox[DONE_SLOT[SELF], :, p * half:(p + 1) * half]
                    split_copy(SELF, inbox.at[DONE_SLOT[SELF]], 1, None).start()
                if k == N_BACK - 1:
                    run_legs(GROUPS[2 * N_CHUNK + N_BACK])
                for o in BACK_ORDER[k * COMBINE_PER:(k + 1) * COMBINE_PER]:
                    j = BACK_SLOT[o]
                    if o != SELF:
                        part(asend.at[j], arecv.at[j]).wait_recv()
                    part(bsend.at[j], brecv.at[j]).wait_recv()
        n = ids.shape[1]
        z = back[pl.ds(g * COMBINE_PER, COMBINE_PER)].reshape(n, half)
        hit = lax.broadcasted_iota(jnp.int32, (n_tok, n), 0).astype(jnp.float32) == ids[pl.ds(g, 1), :]
        left = gts[pl.ds(g, 1), :]
        total = None
        for _ in range(3):
            piece = left.astype(jnp.bfloat16)
            left = left - piece.astype(jnp.float32)
            mat = jnp.where(hit, piece.astype(jnp.float32), 0.0).astype(jnp.bfloat16)
            term = jnp.dot(mat, z, preferred_element_type=jnp.float32)
            total = term if total is None else total + term

        @pl.when(g == 0)
        def _():
            acc[...] = total

        @pl.when(g > 0)
        def _():
            acc[...] += total
        return c

    lax.fori_loop(0, N_BACK, combine, 0)
    n_part = osend.shape[0]
    size = n_tok // n_part

    def out_copies(b):
        at = pl.ds(pl.multiple_of(b * size, size), size)
        src, dst = obuf.at[at], out_ref.at[at, mine]
        return (pltpu.make_async_copy(src, dst, osem.at[b]),
                pltpu.make_async_remote_copy(src, dst, osend.at[b], orecv.at[b], device_id={"tp": other}, device_id_type=MESH))

    def finish(b, c):
        at = pl.ds(pl.multiple_of(b * size, size), size)
        for p in range(n_par):
            @pl.when(core == p)
            def _():
                obuf[at, :] = (x_ref[at, p * half:(p + 1) * half].astype(jnp.float32) + acc[at, :]).astype(jnp.bfloat16)
        for copy in out_copies(b):
            copy.start()
        return c

    lax.fori_loop(0, n_part, finish, 0)

    def drain_legs(k, c):
        whole(send.at[k], recv.at[0]).wait_send()
        return c

    lax.fori_loop(0, len(OUT_LEGS), drain_legs, 0)

    def drain_vals(j, c):
        pltpu.make_async_remote_copy(rval.at[0], rval.at[0], vsend.at[j], vrecv.at[0], device_id={"tp": other}, device_id_type=MESH).wait_send()
        return c

    lax.fori_loop(0, len(OFFSETS), drain_vals, 0)
    for _, o, _, i in BACK_LEGS:
        if i < N_LEGS[o] - 1:
            whole(rsend.at[BACK_ID[o, i]], rrecv.at[0]).wait_send()

    def drain_back(j, c):
        @pl.when(j != BACK_SLOT[SELF])
        def _():
            part(asend.at[j], arecv.at[j]).wait_send()
        part(bsend.at[j], brecv.at[j]).wait_send()
        return c

    lax.fori_loop(0, n_slot, drain_back, 0)

    def drain_out(b, c):
        for copy in out_copies(b):
            copy.wait()
        return c

    lax.fori_loop(0, n_part, drain_out, 0)


def solution(mesh):
    n_groups = mesh.shape["ep"]
    any_spec = pl.BlockSpec(memory_space=pl.ANY)
    vmem_spec = pl.BlockSpec(memory_space=pltpu.VMEM)
    dma = pltpu.SemaphoreType.DMA
    n_legs, n_jobs = len(OUT_LEGS), len(OFFSETS)

    def local_layer(x_local, logit_local, w_up, w_down):
        n_tok, d_model = x_local.shape
        n_experts = logit_local.shape[1]
        own_experts, _, hid = w_up.shape
        capacity = CAP_FACTOR * n_tok * n_groups // n_experts
        cand = 2 * capacity // n_groups
        half = d_model // 2
        n_back_rows = COMBINE_PER * own_experts * cand
        block = lambda n: pltpu.VMEM((n, cand, d_model), jnp.bfloat16)
        table = pltpu.VMEM((cand, n_experts), jnp.float32)
        score = pltpu.VMEM((n_tok, n_experts), jnp.float32)

        out, _, _ = pl.pallas_call(
            functools.partial(layer_kernel, capacity),
            out_shape=(
                jax.ShapeDtypeStruct((n_tok, d_model), jnp.bfloat16),
                jax.ShapeDtypeStruct((N_HOP[0], cand, d_model), jnp.bfloat16),
                jax.ShapeDtypeStruct((N_HOP[1], cand, d_model), jnp.bfloat16),
            ),
            in_specs=[vmem_spec, any_spec, any_spec, any_spec],
            out_specs=(any_spec,) * 3,
            scratch_shapes=[
                pltpu.VMEM((n_tok, d_model), jnp.bfloat16),
                table, table, table, score, score,
                pltpu.VMEM((n_groups, 1, 128), jnp.float32),
                pltpu.VMEM((n_groups * cand, 1), jnp.float32),
                pltpu.VMEM((N_BACK, n_back_rows), jnp.float32), pltpu.VMEM((N_BACK, n_back_rows), jnp.float32),
                block(n_groups), block(N_HOP[0]), block(N_HOP[1]), block(n_groups),
                pltpu.VMEM((n_groups, 1, 128), jnp.float32),
                pltpu.VMEM((2, d_model, hid), jnp.bfloat16), pltpu.VMEM((2, hid, d_model), jnp.bfloat16),
                pltpu.VMEM((n_groups, own_experts, cand, half), jnp.bfloat16),
                pltpu.VMEM((n_tok, half), jnp.float32), pltpu.VMEM((n_tok, half), jnp.bfloat16),
                dma((n_legs,)), dma((n_legs,)), dma((n_jobs,)), dma((n_jobs,)), dma((2,)), dma((2,)), dma((2,)),
                dma((n_legs,)), dma((n_legs,)), dma((n_groups,)), dma((n_groups,)), dma((n_groups,)), dma((n_groups,)),
                dma((4,)), dma((4,)), dma((4,)), dma,
            ],
            compiler_params=pltpu.CompilerParams(collective_id=0, has_side_effects=True, vmem_limit_bytes=VMEM_LIMIT),
        )(logit_local, x_local, w_up, w_down)
        return out

    token_spec = P(("dp", "ep"), None)
    return jax.shard_map(local_layer, mesh=mesh, in_specs=(token_spec, token_spec, P("ep", None, "tp"), P("ep", "tp", None)), out_specs=token_spec, check_vma=False)
```

```python
import functools

import jax
import jax.numpy as jnp
from jax import lax
from jax.experimental import pallas as pl
from jax.experimental.pallas import tpu as pltpu
from jax.sharding import PartitionSpec as P

CAP_FACTOR = 2
MESH = pl.DeviceIdType.MESH
SIDE = 4
LAG = 10.0
EARLY = 8.0
EARLY_HOP = 8.0
AHEAD = 2.0
DONE_LAG = 5.0
EXPERT_COST = 3.5
PICK_PER, EXPERT_PER, COMBINE_PER = 8, 8, 4
VMEM_LIMIT = 67043328
SELF = (0, 0, 0)


def neg(off):
    return tuple((-v) % SIDE for v in off)


def plan(priority, lag, release, begin):
    jobs = [(p // 16, p // 4 % 4, p % 4) for p in priority]
    dur = {1: 1.0, 3: 1.0, 2: 2.0}
    rem = {o: {d for d in range(3) if o[d]} for o in jobs}
    ready = dict(release)
    count = {o: 0 for o in jobs}
    free = list(begin)
    legs = []
    while any(rem.values()):
        d = min((d for d in range(3) if any(d in rem[o] for o in jobs)), key=lambda d: free[d])
        cand = [o for o in jobs if d in rem[o]]
        avail = [o for o in cand if ready[o] <= free[d] + 1e-9]
        if not avail:
            free[d] = min(ready[o] for o in cand)
            continue
        o = avail[0]
        rem[o].discard(d)
        legs.append((free[d], o, d, count[o]))
        count[o] += 1
        free[d] += dur[o[d]]
        ready[o] = free[d] + lag
    return sorted(legs), {o: ready[o] - lag for o in jobs}, free


OUT_PRIORITY = (47, 11, 14, 4, 51, 20, 56, 18, 1, 48, 62, 29, 44, 16, 37, 30, 10, 19, 12, 33, 63, 49, 9, 17, 25, 5, 32, 50, 36, 15, 57, 38, 52, 53, 2, 3, 21, 23, 8, 22, 26, 45, 7, 31, 59, 27, 43, 46, 54, 42, 55, 28, 35, 41, 6, 39, 58, 40, 61, 60, 24, 13, 34)
BACK_PRIORITY = (10, 4, 39, 12, 16, 63, 27, 47, 7, 38, 21, 8, 51, 60, 44, 24, 11, 1, 29, 18, 55, 50, 35, 20, 23, 41, 62, 36, 56, 48, 45, 59, 15, 58, 31, 43, 61, 26, 32, 19, 49, 14, 25, 53, 2, 46, 9, 52, 34, 17, 6, 22, 3, 54, 37, 30, 40, 42, 57, 5, 28, 13, 33)
OFFSETS = [(a, b, c) for a in range(SIDE) for b in range(SIDE) for c in range(SIDE) if a or b or c]
N_LEGS = {o: sum(1 for v in o if v) for o in OFFSETS}
JOB_ID = {o: j for j, o in enumerate(sorted(OFFSETS, key=lambda o: (-N_LEGS[o], o)))}
N_HOP = [sum(1 for o in OFFSETS if N_LEGS[o] > i) for i in (1, 2)]

OUT_LEGS, OUT_DONE, AXIS_FREE = plan(OUT_PRIORITY, LAG, {o: 0.0 for o in OFFSETS}, (0.0, 0.0, 0.0))
START = {o: t for t, o, _, i in OUT_LEGS if i == 0}
SEND_ORDER = sorted(OFFSETS, key=lambda o: (START[o], o)) + [SELF]
DONE_ORDER = [SELF] + sorted(OFFSETS, key=lambda o: (OUT_DONE[o], o))
SEND_SLOT = {o: p for p, o in enumerate(SEND_ORDER)}
DONE_SLOT = {o: r for r, o in enumerate(DONE_ORDER)}
LEG_ID = {(o, i): k for k, (_, o, _, i) in enumerate(OUT_LEGS)}
N_CHUNK = len(DONE_ORDER) // EXPERT_PER
N_BACK = len(DONE_ORDER) // COMBINE_PER


def chunks(order, per):
    return [order[g:g + per] for g in range(0, len(order), per)]


PICK_TIMES = [min(START[o] for o in c if o != SELF) - EARLY - AHEAD for c in chunks(SEND_ORDER, PICK_PER)]
EXPERT_TIMES = []
for group in chunks(DONE_ORDER, EXPERT_PER):
    at = max(OUT_DONE.get(o, 0.0) for o in group) + DONE_LAG
    EXPERT_TIMES.append(max(at, EXPERT_TIMES[-1] + EXPERT_COST) if EXPERT_TIMES else at)
PICK_TIMES = [min(t, EXPERT_TIMES[0] - 1.0 - 0.01 * (N_CHUNK - g)) for g, t in enumerate(PICK_TIMES)]
RELEASE = {o: EXPERT_TIMES[DONE_SLOT[neg(o)] // EXPERT_PER] + EXPERT_COST + EARLY for o in OFFSETS}
BACK_LEGS, BACK_DONE, _ = plan(BACK_PRIORITY, LAG, RELEASE, AXIS_FREE)
BACK_ID = {(o, i): k for k, (_, o, _, i) in enumerate(BACK_LEGS)}
BACK_ORDER = [SELF] + sorted(OFFSETS, key=lambda o: (BACK_DONE[o], o))
BACK_SLOT = {o: r for r, o in enumerate(BACK_ORDER)}
BACK_TIMES = [max(BACK_DONE.get(o, 0.0) for o in c) + DONE_LAG for c in chunks(BACK_ORDER, COMBINE_PER)]
BACK_TIMES = [max(t, EXPERT_TIMES[-1] + EXPERT_COST) for t in BACK_TIMES]


def group_events():
    rest = [(t - (EARLY_HOP if i else EARLY), kind, (o, axis, i)) for kind, legs in ((0, OUT_LEGS), (1, BACK_LEGS)) for t, o, axis, i in legs]
    rest.sort()
    groups = []
    for t in PICK_TIMES + EXPERT_TIMES + BACK_TIMES:
        groups.append([e[1:] for e in rest if e[0] < t])
        rest = [e for e in rest if e[0] >= t]
    return groups + [[e[1:] for e in rest]]


GROUPS = group_events()


def axis_peers(me, sign):
    z = lax.div(me, SIDE * SIDE)
    y = lax.rem(lax.div(me, SIDE), SIDE)
    x = lax.rem(me, SIDE)
    return [[lax.rem(p + v + sign * (2 * SIDE - 2 * v), SIDE) * scale for v in range(SIDE)] for p, scale in ((z, SIDE * SIDE), (y, SIDE), (x, 1))]


def peer_at(table, off):
    return table[0][off[0]] + table[1][off[1]] + table[2][off[2]]


def leg_peer(table, off, axis):
    return peer_at(table, tuple(v if q == axis else 0 for q, v in enumerate(off)))


def lane_column(table, lane):
    lanes = lax.broadcasted_iota(jnp.int32, table.shape, 1)
    return jnp.sum(jnp.where(lanes == lane, table, 0.0), axis=1, keepdims=True)


def route(n_cand, logit_ref, val_ref, idx_ref, work):
    n_tok, lanes = logit_ref.shape
    step = 64
    fold = lambda v: v.reshape(step // 8, 8, lanes)
    best = jnp.full((8, lanes), -jnp.inf, jnp.float32)
    for lo in range(0, n_tok, step):
        v = logit_ref[lo:lo + step, :]
        work[lo:lo + step, :] = v
        best = jnp.maximum(best, jnp.max(fold(v), axis=0))
    row = lax.broadcasted_iota(jnp.int32, (step, lanes), 0).astype(jnp.float32)

    def body(k, best):
        top = jnp.max(best, axis=0, keepdims=True)
        nxt = jnp.full((8, lanes), -jnp.inf, jnp.float32)
        pos = jnp.zeros((8, lanes), jnp.float32)
        for lo in range(0, n_tok, step):
            v = work[lo:lo + step, :]
            hit = v == top
            v = jnp.where(hit, -jnp.inf, v)
            work[lo:lo + step, :] = v
            nxt = jnp.maximum(nxt, jnp.max(fold(v), axis=0))
            pos = pos + jnp.sum(fold(jnp.where(hit, row + float(lo), 0.0)), axis=0)
        val_ref[pl.ds(k, 1), :] = top
        idx_ref[pl.ds(k, 1), :] = jnp.sum(pos, axis=0, keepdims=True)
        return nxt

    lax.fori_loop(0, n_cand, body, best)


def gates(n_cand, logit_ref, idx_ref, gate_ref, soft):
    n_tok, lanes = logit_ref.shape
    step = 64
    for lo in range(0, n_tok, step):
        v = logit_ref[lo:lo + step, :]
        e = jnp.exp(v - jnp.max(v, axis=1, keepdims=True))
        soft[lo:lo + step, :] = e / jnp.sum(e, axis=1, keepdims=True)
    row = lax.broadcasted_iota(jnp.int32, (step, lanes), 0).astype(jnp.float32)

    def body(k, c):
        at = idx_ref[pl.ds(k, 1), :]
        total = jnp.zeros((8, lanes), jnp.float32)
        for lo in range(0, n_tok, step):
            mine = jnp.where(row == at - float(lo), soft[lo:lo + step, :], 0.0)
            total = total + jnp.sum(mine.reshape(step // 8, 8, lanes), axis=0)
        gate_ref[pl.ds(k, 1), :] = jnp.sum(total, axis=0, keepdims=True)
        return c

    lax.fori_loop(0, n_cand, body, 0)


def layer_kernel(capacity, logit_ref, x_hbm, wu_ref, wd_ref, out_ref, back1, back2,
                 x_ref, val_tab, idx_tab, gate_tab, work, soft, vals, cols, ids, gts, outbox, hop1, hop2, inbox, rval, wu, wd, back, acc, obuf,
                 send, recv, vsend, vrecv, wsend, wrecv, lsem, rsend, rrecv, asend, arecv, bsend, brecv, osend, orecv, osem, xsem):
    me, core = lax.axis_index("ep"), lax.axis_index("tp")
    other = 1 - core
    table = axis_peers(me, core)
    tables = [axis_peers(me, p) for p in range(back.shape[1])]
    n_slot, cand, d_model = outbox.shape
    n_par, half = back.shape[1], back.shape[3]
    n_tok, lanes = x_ref.shape[0], vals.shape[2]
    own_experts = wu_ref.shape[0]
    rows = EXPERT_PER * cand
    mine = pl.ds(pl.multiple_of(core * half, half), half)
    theirs = pl.ds(pl.multiple_of(other * half, half), half)
    hops, back_hops = (hop1, hop2), (back1, back2)

    barrier = pltpu.get_barrier_semaphore()
    greet = [{"ep": peer_at(table, o)} for o in OFFSETS]
    greet += [{"ep": peer_at(table, o), "tp": other} for o in OFFSETS if N_LEGS[o] == 1] + [{"tp": other}]
    for there in greet:
        pl.semaphore_signal(barrier, inc=1, device_id=there, device_id_type=MESH)
    x_copy = pltpu.make_async_copy(x_hbm, x_ref, xsem)
    x_copy.start()
    route(cand, logit_ref, val_tab, idx_tab, work)

    weights = []
    for i, (src, dst) in enumerate(((wu_ref, wu), (wd_ref, wd))):
        weights.append(pltpu.make_async_copy(src.at[core], dst.at[0], lsem.at[i]))
        weights.append(pltpu.make_async_remote_copy(src.at[other], dst.at[1], wsend.at[i], wrecv.at[i], device_id={"tp": other}, device_id_type=MESH))
    def val_copy(o):
        to = peer_at(table, o)
        j = JOB_ID[o]
        return pltpu.make_async_remote_copy(vals.at[SEND_SLOT[o]], rval.at[DONE_SLOT[o]], vsend.at[j], vrecv.at[j], device_id={"ep": to}, device_id_type=MESH)

    def whole(s, r):
        return pltpu.make_async_remote_copy(inbox.at[0], inbox.at[0], s, r, device_id={"tp": other}, device_id_type=MESH)

    def part(s, r):
        return pltpu.make_async_remote_copy(back.at[0, 0], back.at[0, 0], s, r, device_id={"tp": other}, device_id_type=MESH)

    def out_leg(o, axis, i):
        if i:
            whole(send.at[0], recv.at[LEG_ID[o, i - 1]]).wait_recv()
        src = hops[i - 1].at[JOB_ID[o]] if i else outbox.at[SEND_SLOT[o]]
        dst = inbox.at[DONE_SLOT[o]] if i == N_LEGS[o] - 1 else hops[i].at[JOB_ID[o]]
        k = LEG_ID[o, i]
        pltpu.make_async_remote_copy(src, dst, send.at[k], recv.at[k], device_id={"ep": leg_peer(table, o, axis)}, device_id_type=MESH).start()

    def split_copy(o, src, h, to):
        cols_of, (s, r) = ((mine, (asend, arecv)), (theirs, (bsend, brecv)))[h]
        j = BACK_SLOT[o]
        there = {} if to is None else {"ep": to}
        if h:
            there["tp"] = other
        return pltpu.make_async_remote_copy(src.at[:, cols_of], back.at[j, core], s.at[j], r.at[j], device_id=there, device_id_type=MESH)

    def back_leg(o, axis, i):
        if i:
            whole(rsend.at[0], rrecv.at[BACK_ID[o, i - 1]]).wait_recv()
        src = back_hops[i - 1].at[JOB_ID[o]] if i else inbox.at[DONE_SLOT[neg(o)]]
        to = leg_peer(table, o, axis)
        if i == N_LEGS[o] - 1:
            for h in range(2):
                split_copy(o, src, h, to).start()
        else:
            k = BACK_ID[o, i]
            pltpu.make_async_remote_copy(src, back_hops[i].at[JOB_ID[o]], rsend.at[k], rrecv.at[k], device_id={"ep": to}, device_id_type=MESH).start()

    def run_legs(group):
        for kind, leg in group:
            (back_leg if kind else out_leg)(*leg)

    val, idx = val_tab[...], idx_tab[...]
    pack = lanes // cand
    slot_row = lax.broadcasted_iota(jnp.int32, (cand, lanes), 0)
    slot_lane = lax.broadcasted_iota(jnp.int32, (cand, lanes), 1)

    def set_columns(p):
        e = own_experts * peer_at(table, SEND_ORDER[p]) + core
        cols[p * cand:(p + 1) * cand, :] = lane_column(idx, e)
        at = DONE_SLOT[SEND_ORDER[p]] % pack * cand
        vals[p] = jnp.sum(jnp.where(slot_lane == slot_row + at, lane_column(val, e), 0.0), axis=0, keepdims=True)

    def set_rows(g):
        at = []
        for o in BACK_ORDER[g * COMBINE_PER:(g + 1) * COMBINE_PER]:
            for p in range(n_par):
                at.append(own_experts * peer_at(tables[p], neg(o)) + p)
        n = len(at) * cand
        eye = lax.broadcasted_iota(jnp.int32, (n, n), 0) == lax.broadcasted_iota(jnp.int32, (n, n), 1)
        for source, dst in ((idx, ids), (gate_tab[...], gts)):
            col = jnp.concatenate([lane_column(source, e) for e in at], axis=0)
            dst[g:g + 1, :] = jnp.sum(jnp.where(eye, col, 0.0), axis=0, keepdims=True)

    for p in range(PICK_PER):
        set_columns(p)
    x_copy.wait()

    def gather(g):
        at = pl.multiple_of(g * rows, rows)
        onehot = (lax.broadcasted_iota(jnp.int32, (rows, n_tok), 1).astype(jnp.float32) == cols[pl.ds(at, rows), :]).astype(jnp.bfloat16)
        got = jnp.dot(onehot, x_ref[...], preferred_element_type=jnp.float32).astype(jnp.bfloat16)
        outbox[pl.ds(g * PICK_PER, PICK_PER)] = got.reshape(PICK_PER, cand, d_model)

    half_way = N_CHUNK // 2
    gather(0)
    pl.semaphore_wait(barrier, len(greet))

    def pick(g, c):
        for k in range(1, N_CHUNK):
            @pl.when(g == k)
            def _():
                run_legs(GROUPS[0] + GROUPS[1] if k == 1 else GROUPS[k])
                if k == 1:
                    for w in weights:
                        w.start()
                for p in range(k * PICK_PER, (k + 1) * PICK_PER):
                    if k <= half_way:
                        set_columns(p)
        gather(g)
        for k in range(1, N_CHUNK):
            @pl.when(g == k)
            def _():
                if k == half_way:
                    for p in range((k + 1) * PICK_PER, n_slot):
                        set_columns(p)
                    for o in OFFSETS:
                        val_copy(o).start()
                    gates(cand, logit_ref, idx_tab, gate_tab, soft)
                if k >= half_way:
                    share = N_BACK // (N_CHUNK - half_way)
                    for b in range((k - half_way) * share, (k - half_way + 1) * share):
                        set_rows(b)
        return c

    lax.fori_loop(1, N_CHUNK, pick, 0)
    inbox[DONE_SLOT[SELF]] = outbox[SEND_SLOT[SELF]]
    rval[DONE_SLOT[SELF]] = vals[SEND_SLOT[SELF]]

    def expert(g, c):
        for k in range(N_CHUNK):
            @pl.when(g == k)
            def _():
                run_legs(GROUPS[N_CHUNK + k])
                if k == 0:
                    for o in OFFSETS:
                        val_copy(o).wait_recv()
                    for w in weights:
                        w.wait()
                for o in DONE_ORDER[k * EXPERT_PER:(k + 1) * EXPERT_PER]:
                    if o != SELF:
                        whole(send.at[0], recv.at[LEG_ID[o, N_LEGS[o] - 1]]).wait_recv()
        own = lax.rem(slot_lane, cand) == slot_row
        value = jnp.concatenate([jnp.sum(jnp.where(own, rval[g * EXPERT_PER + i], 0.0), axis=1, keepdims=True) for i in range(EXPERT_PER)], axis=0)

        def count(j, total):
            packed = rval[j * pack]
            for i in range(1, pack):
                packed = packed + rval[j * pack + i]
            return total + (packed > value).astype(jnp.float32)

        above = lax.fori_loop(0, n_slot // pack, count, jnp.zeros((rows, lanes), jnp.float32), unroll=4)
        keep = jnp.sum(above, axis=1, keepdims=True) < float(capacity)
        here = pl.ds(g * EXPERT_PER, EXPERT_PER)
        x = inbox[here].reshape(rows, d_model)
        z = None
        for h in range(2):
            pre = jnp.dot(x, wu[h], preferred_element_type=jnp.float32)
            hid = jax.nn.gelu(pre, approximate=True).astype(jnp.bfloat16)
            term = jnp.dot(hid, wd[h], preferred_element_type=jnp.float32)
            z = term if z is None else z + term
        inbox[here] = jnp.where(keep, z, 0.0).astype(jnp.bfloat16).reshape(EXPERT_PER, cand, d_model)
        return c

    lax.fori_loop(0, N_CHUNK, expert, 0)

    def await_rows(k):
        run_legs(GROUPS[2 * N_CHUNK + k])
        if k == 0:
            for p in range(n_par):
                @pl.when(core == p)
                def _():
                    back[BACK_SLOT[SELF], p] = inbox[DONE_SLOT[SELF], :, p * half:(p + 1) * half]
            split_copy(SELF, inbox.at[DONE_SLOT[SELF]], 1, None).start()
        if k == N_BACK - 1:
            run_legs(GROUPS[2 * N_CHUNK + N_BACK])
        for o in BACK_ORDER[k * COMBINE_PER:(k + 1) * COMBINE_PER]:
            j = BACK_SLOT[o]
            if o != SELF:
                part(asend.at[j], arecv.at[j]).wait_recv()
            part(bsend.at[j], brecv.at[j]).wait_recv()

    def gated_sum(g, first, count):
        n = ids.shape[1]
        z = back[pl.ds(g * COMBINE_PER, COMBINE_PER)].reshape(n, half)
        token = lax.broadcasted_iota(jnp.int32, (count, n), 0) + first
        hit = token.astype(jnp.float32) == ids[pl.ds(g, 1), :]
        left = gts[pl.ds(g, 1), :]
        total = None
        for _ in range(3):
            piece = left.astype(jnp.bfloat16)
            left = left - piece.astype(jnp.float32)
            mat = jnp.where(hit, piece.astype(jnp.float32), 0.0).astype(jnp.bfloat16)
            term = jnp.dot(mat, z, preferred_element_type=jnp.float32)
            total = term if total is None else total + term
        return total

    def combine(g, c):
        for k in range(N_BACK - 1):
            @pl.when(g == k)
            def _():
                await_rows(k)
        total = gated_sum(g, 0, n_tok)

        @pl.when(g == 0)
        def _():
            acc[...] = total

        @pl.when(g > 0)
        def _():
            acc[...] += total
        return c

    lax.fori_loop(0, N_BACK - 1, combine, 0)
    await_rows(N_BACK - 1)
    n_part = osend.shape[0]
    size = n_tok // n_part

    def out_copies(b):
        at = pl.ds(pl.multiple_of(b * size, size), size)
        src, dst = obuf.at[at], out_ref.at[at, mine]
        return (pltpu.make_async_copy(src, dst, osem.at[b]),
                pltpu.make_async_remote_copy(src, dst, osend.at[b], orecv.at[b], device_id={"tp": other}, device_id_type=MESH))

    def finish(b, c):
        at = pl.ds(pl.multiple_of(b * size, size), size)
        y = acc[at, :] + gated_sum(N_BACK - 1, b * size, size)
        for p in range(n_par):
            @pl.when(core == p)
            def _():
                obuf[at, :] = (x_ref[at, p * half:(p + 1) * half].astype(jnp.float32) + y).astype(jnp.bfloat16)
        for copy in out_copies(b):
            copy.start()
        return c

    lax.fori_loop(0, n_part, finish, 0)

    def drain_legs(k, c):
        whole(send.at[k], recv.at[0]).wait_send()
        return c

    lax.fori_loop(0, len(OUT_LEGS), drain_legs, 0)

    def drain_vals(j, c):
        pltpu.make_async_remote_copy(rval.at[0], rval.at[0], vsend.at[j], vrecv.at[0], device_id={"tp": other}, device_id_type=MESH).wait_send()
        return c

    lax.fori_loop(0, len(OFFSETS), drain_vals, 0)
    for _, o, _, i in BACK_LEGS:
        if i < N_LEGS[o] - 1:
            whole(rsend.at[BACK_ID[o, i]], rrecv.at[0]).wait_send()

    def drain_back(j, c):
        @pl.when(j != BACK_SLOT[SELF])
        def _():
            part(asend.at[j], arecv.at[j]).wait_send()
        part(bsend.at[j], brecv.at[j]).wait_send()
        return c

    lax.fori_loop(0, n_slot, drain_back, 0)

    def drain_out(b, c):
        for copy in out_copies(b):
            copy.wait()
        return c

    lax.fori_loop(0, n_part, drain_out, 0)


def solution(mesh):
    n_groups = mesh.shape["ep"]
    any_spec = pl.BlockSpec(memory_space=pl.ANY)
    vmem_spec = pl.BlockSpec(memory_space=pltpu.VMEM)
    dma = pltpu.SemaphoreType.DMA
    n_legs, n_jobs = len(OUT_LEGS), len(OFFSETS)

    def local_layer(x_local, logit_local, w_up, w_down):
        n_tok, d_model = x_local.shape
        n_experts = logit_local.shape[1]
        own_experts, _, hid = w_up.shape
        capacity = CAP_FACTOR * n_tok * n_groups // n_experts
        cand = 2 * capacity // n_groups
        half = d_model // 2
        n_back_rows = COMBINE_PER * own_experts * cand
        block = lambda n: pltpu.VMEM((n, cand, d_model), jnp.bfloat16)
        table = pltpu.VMEM((cand, n_experts), jnp.float32)
        score = pltpu.VMEM((n_tok, n_experts), jnp.float32)

        out, _, _ = pl.pallas_call(
            functools.partial(layer_kernel, capacity),
            out_shape=(
                jax.ShapeDtypeStruct((n_tok, d_model), jnp.bfloat16),
                jax.ShapeDtypeStruct((N_HOP[0], cand, d_model), jnp.bfloat16),
                jax.ShapeDtypeStruct((N_HOP[1], cand, d_model), jnp.bfloat16),
            ),
            in_specs=[vmem_spec, any_spec, any_spec, any_spec],
            out_specs=(any_spec,) * 3,
            scratch_shapes=[
                pltpu.VMEM((n_tok, d_model), jnp.bfloat16),
                table, table, table, score, score,
                pltpu.VMEM((n_groups, 1, 128), jnp.float32),
                pltpu.VMEM((n_groups * cand, 1), jnp.float32),
                pltpu.VMEM((N_BACK, n_back_rows), jnp.float32), pltpu.VMEM((N_BACK, n_back_rows), jnp.float32),
                block(n_groups), block(N_HOP[0]), block(N_HOP[1]), block(n_groups),
                pltpu.VMEM((n_groups, 1, 128), jnp.float32),
                pltpu.VMEM((2, d_model, hid), jnp.bfloat16), pltpu.VMEM((2, hid, d_model), jnp.bfloat16),
                pltpu.VMEM((n_groups, own_experts, cand, half), jnp.bfloat16),
                pltpu.VMEM((n_tok, half), jnp.float32), pltpu.VMEM((n_tok, half), jnp.bfloat16),
                dma((n_legs,)), dma((n_legs,)), dma((n_jobs,)), dma((n_jobs,)), dma((2,)), dma((2,)), dma((2,)),
                dma((n_legs,)), dma((n_legs,)), dma((n_groups,)), dma((n_groups,)), dma((n_groups,)), dma((n_groups,)),
                dma((4,)), dma((4,)), dma((4,)), dma,
            ],
            compiler_params=pltpu.CompilerParams(collective_id=0, has_side_effects=True, vmem_limit_bytes=VMEM_LIMIT),
        )(logit_local, x_local, w_up, w_down)
        return out

    token_spec = P(("dp", "ep"), None)
    return jax.shard_map(local_layer, mesh=mesh, in_specs=(token_spec, token_spec, P("ep", None, "tp"), P("ep", "tp", None)), out_specs=token_spec, check_vma=False)
```

```python
import functools

import jax
import jax.numpy as jnp
from jax import lax
from jax.experimental import pallas as pl
from jax.experimental.pallas import tpu as pltpu
from jax.sharding import PartitionSpec as P

CAP_FACTOR = 2
MESH = pl.DeviceIdType.MESH
SIDE = 4
LAG = 10.0
EARLY = 8.0
EARLY_HOP = 8.0
AHEAD = 2.0
DONE_LAG = 5.0
EXPERT_COST = 3.5
PICK_PER, EXPERT_PER, COMBINE_PER = 8, 8, 4
VMEM_LIMIT = 59 * 1024 * 1024
SELF = (0, 0, 0)


def neg(off):
    return tuple((-v) % SIDE for v in off)


def plan(priority, lag, release, begin):
    jobs = [(p // 16, p // 4 % 4, p % 4) for p in priority]
    dur = {1: 1.0, 3: 1.0, 2: 2.0}
    rem = {o: {d for d in range(3) if o[d]} for o in jobs}
    ready = dict(release)
    count = {o: 0 for o in jobs}
    free = list(begin)
    legs = []
    while any(rem.values()):
        d = min((d for d in range(3) if any(d in rem[o] for o in jobs)), key=lambda d: free[d])
        cand = [o for o in jobs if d in rem[o]]
        avail = [o for o in cand if ready[o] <= free[d] + 1e-9]
        if not avail:
            free[d] = min(ready[o] for o in cand)
            continue
        o = avail[0]
        rem[o].discard(d)
        legs.append((free[d], o, d, count[o]))
        count[o] += 1
        free[d] += dur[o[d]]
        ready[o] = free[d] + lag
    return sorted(legs), {o: ready[o] - lag for o in jobs}, free


OUT_PRIORITY = (47, 11, 14, 4, 51, 20, 56, 18, 1, 48, 62, 29, 44, 16, 37, 30, 10, 19, 12, 33, 63, 49, 9, 17, 25, 5, 32, 50, 36, 15, 57, 38, 52, 53, 2, 3, 21, 23, 8, 22, 26, 45, 7, 31, 59, 27, 43, 46, 54, 42, 55, 28, 35, 41, 6, 39, 58, 40, 61, 60, 24, 13, 34)
BACK_PRIORITY = (10, 4, 39, 12, 16, 63, 27, 47, 7, 38, 21, 8, 51, 60, 44, 24, 11, 1, 29, 18, 55, 50, 35, 20, 23, 41, 62, 36, 56, 48, 45, 59, 15, 58, 31, 43, 61, 26, 32, 19, 49, 14, 25, 53, 2, 46, 9, 52, 34, 17, 6, 22, 3, 54, 37, 30, 40, 42, 57, 5, 28, 13, 33)
OFFSETS = [(a, b, c) for a in range(SIDE) for b in range(SIDE) for c in range(SIDE) if a or b or c]
N_LEGS = {o: sum(1 for v in o if v) for o in OFFSETS}
JOB_ID = {o: j for j, o in enumerate(sorted(OFFSETS, key=lambda o: (-N_LEGS[o], o)))}
N_HOP = [sum(1 for o in OFFSETS if N_LEGS[o] > i) for i in (1, 2)]

OUT_LEGS, OUT_DONE, AXIS_FREE = plan(OUT_PRIORITY, LAG, {o: 0.0 for o in OFFSETS}, (0.0, 0.0, 0.0))
START = {o: t for t, o, _, i in OUT_LEGS if i == 0}
SEND_ORDER = sorted(OFFSETS, key=lambda o: (START[o], o)) + [SELF]
DONE_ORDER = [SELF] + sorted(OFFSETS, key=lambda o: (OUT_DONE[o], o))
SEND_SLOT = {o: p for p, o in enumerate(SEND_ORDER)}
DONE_SLOT = {o: r for r, o in enumerate(DONE_ORDER)}
LEG_ID = {(o, i): k for k, (_, o, _, i) in enumerate(OUT_LEGS)}
N_CHUNK = len(DONE_ORDER) // EXPERT_PER
N_BACK = len(DONE_ORDER) // COMBINE_PER


def chunks(order, per):
    return [order[g:g + per] for g in range(0, len(order), per)]


PICK_TIMES = [min(START[o] for o in c if o != SELF) - EARLY - AHEAD for c in chunks(SEND_ORDER, PICK_PER)]
EXPERT_TIMES = []
for group in chunks(DONE_ORDER, EXPERT_PER):
    at = max(OUT_DONE.get(o, 0.0) for o in group) + DONE_LAG
    EXPERT_TIMES.append(max(at, EXPERT_TIMES[-1] + EXPERT_COST) if EXPERT_TIMES else at)
PICK_TIMES = [min(t, EXPERT_TIMES[0] - 1.0 - 0.01 * (N_CHUNK - g)) for g, t in enumerate(PICK_TIMES)]
RELEASE = {o: EXPERT_TIMES[DONE_SLOT[neg(o)] // EXPERT_PER] + EXPERT_COST + EARLY for o in OFFSETS}
BACK_LEGS, BACK_DONE, _ = plan(BACK_PRIORITY, LAG, RELEASE, AXIS_FREE)
BACK_ID = {(o, i): k for k, (_, o, _, i) in enumerate(BACK_LEGS)}
BACK_ORDER = [SELF] + sorted(OFFSETS, key=lambda o: (BACK_DONE[o], o))
BACK_SLOT = {o: r for r, o in enumerate(BACK_ORDER)}
BACK_TIMES = [max(BACK_DONE.get(o, 0.0) for o in c) + DONE_LAG for c in chunks(BACK_ORDER, COMBINE_PER)]
BACK_TIMES = [max(t, EXPERT_TIMES[-1] + EXPERT_COST) for t in BACK_TIMES]


def group_events():
    rest = [(t - (EARLY_HOP if i else EARLY), kind, (o, axis, i)) for kind, legs in ((0, OUT_LEGS), (1, BACK_LEGS)) for t, o, axis, i in legs]
    rest.sort()
    groups = []
    for t in PICK_TIMES + EXPERT_TIMES + BACK_TIMES:
        groups.append([e[1:] for e in rest if e[0] < t])
        rest = [e for e in rest if e[0] >= t]
    return groups + [[e[1:] for e in rest]]


GROUPS = group_events()


def axis_peers(me, sign):
    z = lax.div(me, SIDE * SIDE)
    y = lax.rem(lax.div(me, SIDE), SIDE)
    x = lax.rem(me, SIDE)
    return [[lax.rem(p + v + sign * (2 * SIDE - 2 * v), SIDE) * scale for v in range(SIDE)] for p, scale in ((z, SIDE * SIDE), (y, SIDE), (x, 1))]


def peer_at(table, off):
    return table[0][off[0]] + table[1][off[1]] + table[2][off[2]]


def leg_peer(table, off, axis):
    return peer_at(table, tuple(v if q == axis else 0 for q, v in enumerate(off)))


def lane_column(table, lane):
    lanes = lax.broadcasted_iota(jnp.int32, table.shape, 1)
    return jnp.sum(jnp.where(lanes == lane, table, 0.0), axis=1, keepdims=True)


def route(n_cand, logit_ref, val_ref, idx_ref, work):
    n_tok, lanes = logit_ref.shape
    step = 64
    fold = lambda v: v.reshape(step // 8, 8, lanes)
    best = jnp.full((8, lanes), -jnp.inf, jnp.float32)
    for lo in range(0, n_tok, step):
        v = logit_ref[lo:lo + step, :]
        work[lo:lo + step, :] = v
        best = jnp.maximum(best, jnp.max(fold(v), axis=0))
    row = lax.broadcasted_iota(jnp.int32, (step, lanes), 0).astype(jnp.float32)

    def body(k, best):
        top = jnp.max(best, axis=0, keepdims=True)
        nxt = jnp.full((8, lanes), -jnp.inf, jnp.float32)
        pos = jnp.zeros((8, lanes), jnp.float32)
        for lo in range(0, n_tok, step):
            v = work[lo:lo + step, :]
            hit = v == top
            v = jnp.where(hit, -jnp.inf, v)
            work[lo:lo + step, :] = v
            nxt = jnp.maximum(nxt, jnp.max(fold(v), axis=0))
            pos = pos + jnp.sum(fold(jnp.where(hit, row + float(lo), 0.0)), axis=0)
        val_ref[pl.ds(k, 1), :] = top
        idx_ref[pl.ds(k, 1), :] = jnp.sum(pos, axis=0, keepdims=True)
        return nxt

    lax.fori_loop(0, n_cand, body, best)


def gates(n_cand, logit_ref, idx_ref, gate_ref, soft):
    n_tok, lanes = logit_ref.shape
    step = 64
    for lo in range(0, n_tok, step):
        v = logit_ref[lo:lo + step, :]
        e = jnp.exp(v - jnp.max(v, axis=1, keepdims=True))
        soft[lo:lo + step, :] = e / jnp.sum(e, axis=1, keepdims=True)
    row = lax.broadcasted_iota(jnp.int32, (step, lanes), 0).astype(jnp.float32)

    def body(k, c):
        at = idx_ref[pl.ds(k, 1), :]
        total = jnp.zeros((8, lanes), jnp.float32)
        for lo in range(0, n_tok, step):
            mine = jnp.where(row == at - float(lo), soft[lo:lo + step, :], 0.0)
            total = total + jnp.sum(mine.reshape(step // 8, 8, lanes), axis=0)
        gate_ref[pl.ds(k, 1), :] = jnp.sum(total, axis=0, keepdims=True)
        return c

    lax.fori_loop(0, n_cand, body, 0)


def layer_kernel(capacity, logit_ref, x_hbm, wu_ref, wd_ref, out_ref, back1, back2,
                 x_ref, val_tab, idx_tab, gate_tab, work, soft, vals, cols, ids, gts, outbox, hop1, hop2, inbox, rval, wu, wd, back, acc,
                 send, recv, vsend, vrecv, wsend, wrecv, lsem, rsend, rrecv, asend, arecv, bsend, brecv, osend, orecv, xsem):
    me, core = lax.axis_index("ep"), lax.axis_index("tp")
    other = 1 - core
    table = axis_peers(me, core)
    tables = [axis_peers(me, p) for p in range(back.shape[1])]
    n_slot, cand, d_model = outbox.shape
    n_par, half = back.shape[1], back.shape[3]
    n_tok, lanes = x_ref.shape[0], vals.shape[2]
    own_experts = wu_ref.shape[0]
    rows = EXPERT_PER * cand
    mine = pl.ds(pl.multiple_of(core * half, half), half)
    theirs = pl.ds(pl.multiple_of(other * half, half), half)
    hops, back_hops = (hop1, hop2), (back1, back2)

    barrier = pltpu.get_barrier_semaphore()
    greet = [{"ep": peer_at(table, o)} for o in OFFSETS]
    greet += [{"ep": peer_at(table, o), "tp": other} for o in OFFSETS if N_LEGS[o] == 1] + [{"tp": other}]
    for there in greet:
        pl.semaphore_signal(barrier, inc=1, device_id=there, device_id_type=MESH)
    x_copy = pltpu.make_async_copy(x_hbm, x_ref, xsem)
    x_copy.start()
    route(cand, logit_ref, val_tab, idx_tab, work)

    weights = []
    for i, (src, dst) in enumerate(((wu_ref, wu), (wd_ref, wd))):
        weights.append(pltpu.make_async_copy(src.at[core], dst.at[0], lsem.at[i]))
        weights.append(pltpu.make_async_remote_copy(src.at[other], dst.at[1], wsend.at[i], wrecv.at[i], device_id={"tp": other}, device_id_type=MESH))
    def val_copy(o):
        to = peer_at(table, o)
        j = JOB_ID[o]
        return pltpu.make_async_remote_copy(vals.at[SEND_SLOT[o]], rval.at[DONE_SLOT[o]], vsend.at[j], vrecv.at[j], device_id={"ep": to}, device_id_type=MESH)

    def whole(s, r):
        return pltpu.make_async_remote_copy(inbox.at[0], inbox.at[0], s, r, device_id={"tp": other}, device_id_type=MESH)

    def part(s, r):
        return pltpu.make_async_remote_copy(back.at[0, 0], back.at[0, 0], s, r, device_id={"tp": other}, device_id_type=MESH)

    def out_leg(o, axis, i):
        if i:
            whole(send.at[0], recv.at[LEG_ID[o, i - 1]]).wait_recv()
        src = hops[i - 1].at[JOB_ID[o]] if i else outbox.at[SEND_SLOT[o]]
        dst = inbox.at[DONE_SLOT[o]] if i == N_LEGS[o] - 1 else hops[i].at[JOB_ID[o]]
        k = LEG_ID[o, i]
        pltpu.make_async_remote_copy(src, dst, send.at[k], recv.at[k], device_id={"ep": leg_peer(table, o, axis)}, device_id_type=MESH).start()

    def split_copy(o, src, h, to):
        cols_of, (s, r) = ((mine, (asend, arecv)), (theirs, (bsend, brecv)))[h]
        j = BACK_SLOT[o]
        there = {} if to is None else {"ep": to}
        if h:
            there["tp"] = other
        return pltpu.make_async_remote_copy(src.at[:, cols_of], back.at[j, core], s.at[j], r.at[j], device_id=there, device_id_type=MESH)

    def back_leg(o, axis, i):
        if i:
            whole(rsend.at[0], rrecv.at[BACK_ID[o, i - 1]]).wait_recv()
        src = back_hops[i - 1].at[JOB_ID[o]] if i else inbox.at[DONE_SLOT[neg(o)]]
        to = leg_peer(table, o, axis)
        if i == N_LEGS[o] - 1:
            for h in range(2):
                split_copy(o, src, h, to).start()
        else:
            k = BACK_ID[o, i]
            pltpu.make_async_remote_copy(src, back_hops[i].at[JOB_ID[o]], rsend.at[k], rrecv.at[k], device_id={"ep": to}, device_id_type=MESH).start()

    def run_legs(group):
        for kind, leg in group:
            (back_leg if kind else out_leg)(*leg)

    val, idx = val_tab[...], idx_tab[...]
    pack = lanes // cand
    slot_row = lax.broadcasted_iota(jnp.int32, (cand, lanes), 0)
    slot_lane = lax.broadcasted_iota(jnp.int32, (cand, lanes), 1)

    def set_columns(p):
        e = own_experts * peer_at(table, SEND_ORDER[p]) + core
        cols[p * cand:(p + 1) * cand, :] = lane_column(idx, e)
        at = DONE_SLOT[SEND_ORDER[p]] % pack * cand
        vals[p] = jnp.sum(jnp.where(slot_lane == slot_row + at, lane_column(val, e), 0.0), axis=0, keepdims=True)

    def set_rows(g):
        at = []
        for o in BACK_ORDER[g * COMBINE_PER:(g + 1) * COMBINE_PER]:
            for p in range(n_par):
                at.append(own_experts * peer_at(tables[p], neg(o)) + p)
        n = len(at) * cand
        eye = lax.broadcasted_iota(jnp.int32, (n, n), 0) == lax.broadcasted_iota(jnp.int32, (n, n), 1)
        for source, dst in ((idx, ids), (gate_tab[...], gts)):
            col = jnp.concatenate([lane_column(source, e) for e in at], axis=0)
            dst[g:g + 1, :] = jnp.sum(jnp.where(eye, col, 0.0), axis=0, keepdims=True)

    for p in range(PICK_PER):
        set_columns(p)
    x_copy.wait()

    def gather(g):
        at = pl.multiple_of(g * rows, rows)
        onehot = (lax.broadcasted_iota(jnp.int32, (rows, n_tok), 1).astype(jnp.float32) == cols[pl.ds(at, rows), :]).astype(jnp.bfloat16)
        got = jnp.dot(onehot, x_ref[...], preferred_element_type=jnp.float32).astype(jnp.bfloat16)
        outbox[pl.ds(g * PICK_PER, PICK_PER)] = got.reshape(PICK_PER, cand, d_model)

    half_way = N_CHUNK // 2
    gather(0)
    pl.semaphore_wait(barrier, len(greet))

    def pick(g, c):
        for k in range(1, N_CHUNK):
            @pl.when(g == k)
            def _():
                run_legs(GROUPS[0] + GROUPS[1] if k == 1 else GROUPS[k])
                if k == 1:
                    for w in weights:
                        w.start()
                for p in range(k * PICK_PER, (k + 1) * PICK_PER):
                    if k <= half_way:
                        set_columns(p)
        gather(g)
        for k in range(1, N_CHUNK):
            @pl.when(g == k)
            def _():
                if k == half_way:
                    for p in range((k + 1) * PICK_PER, n_slot):
                        set_columns(p)
                    for o in OFFSETS:
                        val_copy(o).start()
                    gates(cand, logit_ref, idx_tab, gate_tab, soft)
                if k >= half_way:
                    share = N_BACK // (N_CHUNK - half_way)
                    for b in range((k - half_way) * share, (k - half_way + 1) * share):
                        set_rows(b)
        return c

    lax.fori_loop(1, N_CHUNK, pick, 0)
    inbox[DONE_SLOT[SELF]] = outbox[SEND_SLOT[SELF]]
    rval[DONE_SLOT[SELF]] = vals[SEND_SLOT[SELF]]

    def expert(g, c):
        for k in range(N_CHUNK):
            @pl.when(g == k)
            def _():
                run_legs(GROUPS[N_CHUNK + k])
                if k == 0:
                    for o in OFFSETS:
                        val_copy(o).wait_recv()
                    for w in weights:
                        w.wait()
                for o in DONE_ORDER[k * EXPERT_PER:(k + 1) * EXPERT_PER]:
                    if o != SELF:
                        whole(send.at[0], recv.at[LEG_ID[o, N_LEGS[o] - 1]]).wait_recv()
        own = lax.rem(slot_lane, cand) == slot_row
        value = jnp.concatenate([jnp.sum(jnp.where(own, rval[g * EXPERT_PER + i], 0.0), axis=1, keepdims=True) for i in range(EXPERT_PER)], axis=0)

        def count(j, total):
            packed = rval[j * pack]
            for i in range(1, pack):
                packed = packed + rval[j * pack + i]
            return total + (packed > value).astype(jnp.float32)

        above = lax.fori_loop(0, n_slot // pack, count, jnp.zeros((rows, lanes), jnp.float32), unroll=4)
        keep = jnp.sum(above, axis=1, keepdims=True) < float(capacity)
        here = pl.ds(g * EXPERT_PER, EXPERT_PER)
        x = inbox[here].reshape(rows, d_model)
        z = None
        for h in range(2):
            pre = jnp.dot(x, wu[h], preferred_element_type=jnp.float32)
            hid = jax.nn.gelu(pre, approximate=True).astype(jnp.bfloat16)
            term = jnp.dot(hid, wd[h], preferred_element_type=jnp.float32)
            z = term if z is None else z + term
        inbox[here] = jnp.where(keep, z, 0.0).astype(jnp.bfloat16).reshape(EXPERT_PER, cand, d_model)
        return c

    lax.fori_loop(0, N_CHUNK, expert, 0)

    def await_rows(k):
        run_legs(GROUPS[2 * N_CHUNK + k])
        if k == 0:
            for p in range(n_par):
                @pl.when(core == p)
                def _():
                    back[BACK_SLOT[SELF], p] = inbox[DONE_SLOT[SELF], :, p * half:(p + 1) * half]
            split_copy(SELF, inbox.at[DONE_SLOT[SELF]], 1, None).start()
        if k == N_BACK - 1:
            run_legs(GROUPS[2 * N_CHUNK + N_BACK])
        for o in BACK_ORDER[k * COMBINE_PER:(k + 1) * COMBINE_PER]:
            j = BACK_SLOT[o]
            if o != SELF:
                part(asend.at[j], arecv.at[j]).wait_recv()
            part(bsend.at[j], brecv.at[j]).wait_recv()

    def gated_sum(g, first, count):
        n = ids.shape[1]
        z = back[pl.ds(g * COMBINE_PER, COMBINE_PER)].reshape(n, half)
        token = lax.broadcasted_iota(jnp.int32, (count, n), 0) + first
        hit = token.astype(jnp.float32) == ids[pl.ds(g, 1), :]
        left = gts[pl.ds(g, 1), :]
        total = None
        for _ in range(3):
            piece = left.astype(jnp.bfloat16)
            left = left - piece.astype(jnp.float32)
            mat = jnp.where(hit, piece.astype(jnp.float32), 0.0).astype(jnp.bfloat16)
            term = jnp.dot(mat, z, preferred_element_type=jnp.float32)
            total = term if total is None else total + term
        return total

    def combine(g, c):
        for k in range(N_BACK - 1):
            @pl.when(g == k)
            def _():
                await_rows(k)
        total = gated_sum(g, 0, n_tok)

        @pl.when(g == 0)
        def _():
            acc[...] = total

        @pl.when(g > 0)
        def _():
            acc[...] += total
        return c

    lax.fori_loop(0, N_BACK - 1, combine, 0)
    await_rows(N_BACK - 1)
    n_part = osend.shape[0]
    size = n_tok // n_part

    def out_copies(b):
        at = pl.ds(pl.multiple_of(b * size, size), size)
        half_of = out_ref.at[at, mine]
        return (pltpu.make_async_remote_copy(half_of, half_of, osend.at[b], orecv.at[b], device_id={"tp": other}, device_id_type=MESH),)

    def finish(b, c):
        at = pl.ds(pl.multiple_of(b * size, size), size)
        y = acc[at, :] + gated_sum(N_BACK - 1, b * size, size)
        for p in range(n_par):
            @pl.when(core == p)
            def _():
                out_ref[at, p * half:(p + 1) * half] = (x_ref[at, p * half:(p + 1) * half].astype(jnp.float32) + y).astype(jnp.bfloat16)
        for copy in out_copies(b):
            copy.start()
        return c

    lax.fori_loop(0, n_part, finish, 0)

    def drain_legs(k, c):
        whole(send.at[k], recv.at[0]).wait_send()
        return c

    lax.fori_loop(0, len(OUT_LEGS), drain_legs, 0)

    def drain_vals(j, c):
        pltpu.make_async_remote_copy(rval.at[0], rval.at[0], vsend.at[j], vrecv.at[0], device_id={"tp": other}, device_id_type=MESH).wait_send()
        return c

    lax.fori_loop(0, len(OFFSETS), drain_vals, 0)
    for _, o, _, i in BACK_LEGS:
        if i < N_LEGS[o] - 1:
            whole(rsend.at[BACK_ID[o, i]], rrecv.at[0]).wait_send()

    def drain_back(j, c):
        @pl.when(j != BACK_SLOT[SELF])
        def _():
            part(asend.at[j], arecv.at[j]).wait_send()
        part(bsend.at[j], brecv.at[j]).wait_send()
        return c

    lax.fori_loop(0, n_slot, drain_back, 0)

    def drain_out(b, c):
        for copy in out_copies(b):
            copy.wait()
        return c

    lax.fori_loop(0, n_part, drain_out, 0)


def solution(mesh):
    n_groups = mesh.shape["ep"]
    any_spec = pl.BlockSpec(memory_space=pl.ANY)
    vmem_spec = pl.BlockSpec(memory_space=pltpu.VMEM)
    dma = pltpu.SemaphoreType.DMA
    n_legs, n_jobs = len(OUT_LEGS), len(OFFSETS)

    def local_layer(x_local, logit_local, w_up, w_down):
        n_tok, d_model = x_local.shape
        n_experts = logit_local.shape[1]
        own_experts, _, hid = w_up.shape
        capacity = CAP_FACTOR * n_tok * n_groups // n_experts
        cand = 2 * capacity // n_groups
        half = d_model // 2
        n_back_rows = COMBINE_PER * own_experts * cand
        block = lambda n: pltpu.VMEM((n, cand, d_model), jnp.bfloat16)
        table = pltpu.VMEM((cand, n_experts), jnp.float32)
        score = pltpu.VMEM((n_tok, n_experts), jnp.float32)

        out, _, _ = pl.pallas_call(
            functools.partial(layer_kernel, capacity),
            out_shape=(
                pltpu.VMEM((n_tok, d_model), jnp.bfloat16),
                jax.ShapeDtypeStruct((N_HOP[0], cand, d_model), jnp.bfloat16),
                jax.ShapeDtypeStruct((N_HOP[1], cand, d_model), jnp.bfloat16),
            ),
            in_specs=[vmem_spec, any_spec, any_spec, any_spec],
            out_specs=(vmem_spec, any_spec, any_spec),
            scratch_shapes=[
                pltpu.VMEM((n_tok, d_model), jnp.bfloat16),
                table, table, table, score, score,
                pltpu.VMEM((n_groups, 1, 128), jnp.float32),
                pltpu.VMEM((n_groups * cand, 1), jnp.float32),
                pltpu.VMEM((N_BACK, n_back_rows), jnp.float32), pltpu.VMEM((N_BACK, n_back_rows), jnp.float32),
                block(n_groups), block(N_HOP[0]), block(N_HOP[1]), block(n_groups),
                pltpu.VMEM((n_groups, 1, 128), jnp.float32),
                pltpu.VMEM((2, d_model, hid), jnp.bfloat16), pltpu.VMEM((2, hid, d_model), jnp.bfloat16),
                pltpu.VMEM((n_groups, own_experts, cand, half), jnp.bfloat16),
                pltpu.VMEM((n_tok, half), jnp.float32),
                dma((n_legs,)), dma((n_legs,)), dma((n_jobs,)), dma((n_jobs,)), dma((2,)), dma((2,)), dma((2,)),
                dma((n_legs,)), dma((n_legs,)), dma((n_groups,)), dma((n_groups,)), dma((n_groups,)), dma((n_groups,)),
                dma((4,)), dma((4,)), dma,
            ],
            compiler_params=pltpu.CompilerParams(collective_id=0, has_side_effects=True, vmem_limit_bytes=VMEM_LIMIT),
        )(logit_local, x_local, w_up, w_down)
        return out

    token_spec = P(("dp", "ep"), None)
    return jax.shard_map(local_layer, mesh=mesh, in_specs=(token_spec, token_spec, P("ep", None, "tp"), P("ep", "tp", None)), out_specs=token_spec, check_vma=False)
```

```python
import functools

import jax
import jax.numpy as jnp
from jax import lax
from jax.experimental import pallas as pl
from jax.experimental.pallas import tpu as pltpu
from jax.sharding import PartitionSpec as P

CAP_FACTOR = 2
MESH = pl.DeviceIdType.MESH
SIDE = 4
LAG = 12.0
EARLY = 10.0
EARLY_HOP = 8.0
AHEAD = 2.0
DONE_LAG = 5.0
EXPERT_COST = 2.7
PICK_PER, EXPERT_PER, COMBINE_PER = 8, 8, 4
VMEM_LIMIT = 59 * 1024 * 1024
SELF = (0, 0, 0)


def neg(off):
    return tuple((-v) % SIDE for v in off)


def plan(priority, lag, release, begin):
    jobs = [(p // 16, p // 4 % 4, p % 4) for p in priority]
    dur = {1: 1.0, 3: 1.0, 2: 2.0}
    rem = {o: {d for d in range(3) if o[d]} for o in jobs}
    ready = dict(release)
    count = {o: 0 for o in jobs}
    free = list(begin)
    legs = []
    while any(rem.values()):
        d = min((d for d in range(3) if any(d in rem[o] for o in jobs)), key=lambda d: free[d])
        cand = [o for o in jobs if d in rem[o]]
        avail = [o for o in cand if ready[o] <= free[d] + 1e-9]
        if not avail:
            free[d] = min(ready[o] for o in cand)
            continue
        o = avail[0]
        rem[o].discard(d)
        legs.append((free[d], o, d, count[o]))
        count[o] += 1
        free[d] += dur[o[d]]
        ready[o] = free[d] + lag
    return sorted(legs), {o: ready[o] - lag for o in jobs}, free


OUT_PRIORITY = (39, 44, 38, 58, 33, 7, 11, 55, 63, 20, 23, 47, 10, 13, 24, 4, 19, 27, 3, 48, 30, 59, 31, 61, 51, 8, 21, 14, 34, 2, 54, 42, 43, 16, 12, 1, 56, 22, 26, 52, 53, 62, 17, 57, 40, 45, 9, 49, 29, 25, 46, 41, 50, 15, 35, 37, 6, 36, 5, 60, 32, 28, 18)
BACK_PRIORITY = (23, 12, 36, 29, 4, 25, 31, 13, 28, 42, 57, 8, 33, 46, 18, 51, 20, 2, 45, 62, 7, 55, 3, 21, 6, 17, 43, 59, 53, 32, 63, 9, 40, 26, 54, 48, 14, 39, 19, 1, 50, 27, 35, 52, 16, 37, 38, 10, 41, 24, 15, 60, 61, 58, 49, 30, 44, 56, 11, 47, 22, 34, 5)
OFFSETS = [(a, b, c) for a in range(SIDE) for b in range(SIDE) for c in range(SIDE) if a or b or c]
N_LEGS = {o: sum(1 for v in o if v) for o in OFFSETS}
JOB_ID = {o: j for j, o in enumerate(sorted(OFFSETS, key=lambda o: (-N_LEGS[o], o)))}
N_HOP = [sum(1 for o in OFFSETS if N_LEGS[o] > i) for i in (1, 2)]

OUT_LEGS, OUT_DONE, AXIS_FREE = plan(OUT_PRIORITY, LAG, {o: 0.0 for o in OFFSETS}, (0.0, 0.0, 0.0))
START = {o: t for t, o, _, i in OUT_LEGS if i == 0}
SEND_ORDER = sorted(OFFSETS, key=lambda o: (START[o], o)) + [SELF]
DONE_ORDER = [SELF] + sorted(OFFSETS, key=lambda o: (OUT_DONE[o], o))
SEND_SLOT = {o: p for p, o in enumerate(SEND_ORDER)}
DONE_SLOT = {o: r for r, o in enumerate(DONE_ORDER)}
LEG_ID = {(o, i): k for k, (_, o, _, i) in enumerate(OUT_LEGS)}
N_CHUNK = len(DONE_ORDER) // EXPERT_PER
N_BACK = len(DONE_ORDER) // COMBINE_PER


def chunks(order, per):
    return [order[g:g + per] for g in range(0, len(order), per)]


PICK_TIMES = [min(START[o] for o in c if o != SELF) - EARLY - AHEAD for c in chunks(SEND_ORDER, PICK_PER)]
EXPERT_TIMES = []
for group in chunks(DONE_ORDER, EXPERT_PER):
    at = max(OUT_DONE.get(o, 0.0) for o in group) + DONE_LAG
    EXPERT_TIMES.append(max(at, EXPERT_TIMES[-1] + EXPERT_COST) if EXPERT_TIMES else at)
PICK_TIMES = [min(t, EXPERT_TIMES[0] - 1.0 - 0.01 * (N_CHUNK - g)) for g, t in enumerate(PICK_TIMES)]
RELEASE = {o: EXPERT_TIMES[DONE_SLOT[neg(o)] // EXPERT_PER] + EXPERT_COST + EARLY for o in OFFSETS}
BACK_LEGS, BACK_DONE, _ = plan(BACK_PRIORITY, LAG, RELEASE, AXIS_FREE)
BACK_ID = {(o, i): k for k, (_, o, _, i) in enumerate(BACK_LEGS)}
BACK_ORDER = [SELF] + sorted(OFFSETS, key=lambda o: (BACK_DONE[o], o))
BACK_SLOT = {o: r for r, o in enumerate(BACK_ORDER)}
BACK_TIMES = [max(BACK_DONE.get(o, 0.0) for o in c) + DONE_LAG for c in chunks(BACK_ORDER, COMBINE_PER)]
BACK_TIMES = [max(t, EXPERT_TIMES[-1] + EXPERT_COST) for t in BACK_TIMES]


def group_events():
    rest = [(t - (EARLY_HOP if i else EARLY), kind, (o, axis, i)) for kind, legs in ((0, OUT_LEGS), (1, BACK_LEGS)) for t, o, axis, i in legs]
    rest.sort()
    groups = []
    for t in PICK_TIMES + EXPERT_TIMES + BACK_TIMES:
        groups.append([e[1:] for e in rest if e[0] < t])
        rest = [e for e in rest if e[0] >= t]
    return groups + [[e[1:] for e in rest]]


GROUPS = group_events()


def axis_peers(me, sign):
    z = lax.div(me, SIDE * SIDE)
    y = lax.rem(lax.div(me, SIDE), SIDE)
    x = lax.rem(me, SIDE)
    return [[lax.rem(p + v + sign * (2 * SIDE - 2 * v), SIDE) * scale for v in range(SIDE)] for p, scale in ((z, SIDE * SIDE), (y, SIDE), (x, 1))]


def peer_at(table, off):
    return table[0][off[0]] + table[1][off[1]] + table[2][off[2]]


def leg_peer(table, off, axis):
    return peer_at(table, tuple(v if q == axis else 0 for q, v in enumerate(off)))


def lane_column(table, lane):
    lanes = lax.broadcasted_iota(jnp.int32, table.shape, 1)
    return jnp.sum(jnp.where(lanes == lane, table, 0.0), axis=1, keepdims=True)


def route(n_cand, logit_ref, val_ref, idx_ref, work):
    n_tok, lanes = logit_ref.shape
    step = 64
    fold = lambda v: v.reshape(step // 8, 8, lanes)
    best = jnp.full((8, lanes), -jnp.inf, jnp.float32)
    for lo in range(0, n_tok, step):
        v = logit_ref[lo:lo + step, :]
        work[lo:lo + step, :] = v
        best = jnp.maximum(best, jnp.max(fold(v), axis=0))
    row = lax.broadcasted_iota(jnp.int32, (step, lanes), 0).astype(jnp.float32)

    def body(k, best):
        top = jnp.max(best, axis=0, keepdims=True)
        nxt = jnp.full((8, lanes), -jnp.inf, jnp.float32)
        pos = jnp.zeros((8, lanes), jnp.float32)
        for lo in range(0, n_tok, step):
            v = work[lo:lo + step, :]
            hit = v == top
            v = jnp.where(hit, -jnp.inf, v)
            work[lo:lo + step, :] = v
            nxt = jnp.maximum(nxt, jnp.max(fold(v), axis=0))
            pos = pos + jnp.sum(fold(jnp.where(hit, row + float(lo), 0.0)), axis=0)
        val_ref[pl.ds(k, 1), :] = top
        idx_ref[pl.ds(k, 1), :] = jnp.sum(pos, axis=0, keepdims=True)
        return nxt

    lax.fori_loop(0, n_cand, body, best)


def gates(n_cand, logit_ref, idx_ref, gate_ref, soft):
    n_tok, lanes = logit_ref.shape
    step = 64
    for lo in range(0, n_tok, step):
        v = logit_ref[lo:lo + step, :]
        e = jnp.exp(v - jnp.max(v, axis=1, keepdims=True))
        soft[lo:lo + step, :] = e / jnp.sum(e, axis=1, keepdims=True)
    row = lax.broadcasted_iota(jnp.int32, (step, lanes), 0).astype(jnp.float32)

    def body(k, c):
        at = idx_ref[pl.ds(k, 1), :]
        total = jnp.zeros((8, lanes), jnp.float32)
        for lo in range(0, n_tok, step):
            mine = jnp.where(row == at - float(lo), soft[lo:lo + step, :], 0.0)
            total = total + jnp.sum(mine.reshape(step // 8, 8, lanes), axis=0)
        gate_ref[pl.ds(k, 1), :] = jnp.sum(total, axis=0, keepdims=True)
        return c

    lax.fori_loop(0, n_cand, body, 0)


def layer_kernel(capacity, logit_ref, x_hbm, wu_ref, wd_ref, out_ref, back1, back2,
                 x_ref, val_tab, idx_tab, gate_tab, work, soft, vals, cols, ids, gts, outbox, hop1, hop2, inbox, rval, wu, wd, back, acc,
                 send, recv, vsend, vrecv, wsend, wrecv, lsem, rsend, rrecv, asend, arecv, bsend, brecv, osend, orecv, xsem):
    me, core = lax.axis_index("ep"), lax.axis_index("tp")
    other = 1 - core
    table = axis_peers(me, core)
    tables = [axis_peers(me, p) for p in range(back.shape[1])]
    n_slot, cand, d_model = outbox.shape
    n_par, half = back.shape[1], back.shape[3]
    n_tok, lanes = x_ref.shape[0], vals.shape[2]
    own_experts = wu_ref.shape[0]
    rows = EXPERT_PER * cand
    mine = pl.ds(pl.multiple_of(core * half, half), half)
    theirs = pl.ds(pl.multiple_of(other * half, half), half)
    hops, back_hops = (hop1, hop2), (back1, back2)

    barrier = pltpu.get_barrier_semaphore()
    greet = [{"ep": peer_at(table, o)} for o in OFFSETS]
    greet += [{"ep": peer_at(table, o), "tp": other} for o in OFFSETS if N_LEGS[o] == 1] + [{"tp": other}]
    for there in greet:
        pl.semaphore_signal(barrier, inc=1, device_id=there, device_id_type=MESH)
    x_copy = pltpu.make_async_copy(x_hbm, x_ref, xsem)
    x_copy.start()
    route(cand, logit_ref, val_tab, idx_tab, work)

    weights = []
    for i, (src, dst) in enumerate(((wu_ref, wu), (wd_ref, wd))):
        weights.append(pltpu.make_async_copy(src.at[core], dst.at[0], lsem.at[i]))
        weights.append(pltpu.make_async_remote_copy(src.at[other], dst.at[1], wsend.at[i], wrecv.at[i], device_id={"tp": other}, device_id_type=MESH))
    def val_copy(o):
        to = peer_at(table, o)
        j = JOB_ID[o]
        return pltpu.make_async_remote_copy(vals.at[SEND_SLOT[o]], rval.at[DONE_SLOT[o]], vsend.at[j], vrecv.at[j], device_id={"ep": to}, device_id_type=MESH)

    def whole(s, r):
        return pltpu.make_async_remote_copy(inbox.at[0], inbox.at[0], s, r, device_id={"tp": other}, device_id_type=MESH)

    def part(s, r):
        return pltpu.make_async_remote_copy(back.at[0, 0], back.at[0, 0], s, r, device_id={"tp": other}, device_id_type=MESH)

    def out_leg(o, axis, i):
        if i:
            whole(send.at[0], recv.at[LEG_ID[o, i - 1]]).wait_recv()
        src = hops[i - 1].at[JOB_ID[o]] if i else outbox.at[SEND_SLOT[o]]
        dst = inbox.at[DONE_SLOT[o]] if i == N_LEGS[o] - 1 else hops[i].at[JOB_ID[o]]
        k = LEG_ID[o, i]
        pltpu.make_async_remote_copy(src, dst, send.at[k], recv.at[k], device_id={"ep": leg_peer(table, o, axis)}, device_id_type=MESH).start()

    def split_copy(o, src, h, to):
        cols_of, (s, r) = ((mine, (asend, arecv)), (theirs, (bsend, brecv)))[h]
        j = BACK_SLOT[o]
        there = {} if to is None else {"ep": to}
        if h:
            there["tp"] = other
        return pltpu.make_async_remote_copy(src.at[:, cols_of], back.at[j, core], s.at[j], r.at[j], device_id=there, device_id_type=MESH)

    def back_leg(o, axis, i):
        if i:
            whole(rsend.at[0], rrecv.at[BACK_ID[o, i - 1]]).wait_recv()
        src = back_hops[i - 1].at[JOB_ID[o]] if i else inbox.at[DONE_SLOT[neg(o)]]
        to = leg_peer(table, o, axis)
        if i == N_LEGS[o] - 1:
            for h in range(2):
                split_copy(o, src, h, to).start()
        else:
            k = BACK_ID[o, i]
            pltpu.make_async_remote_copy(src, back_hops[i].at[JOB_ID[o]], rsend.at[k], rrecv.at[k], device_id={"ep": to}, device_id_type=MESH).start()

    def run_legs(group):
        for kind, leg in group:
            (back_leg if kind else out_leg)(*leg)

    val, idx = val_tab[...], idx_tab[...]
    pack = lanes // cand
    slot_row = lax.broadcasted_iota(jnp.int32, (cand, lanes), 0)
    slot_lane = lax.broadcasted_iota(jnp.int32, (cand, lanes), 1)

    def set_columns(p):
        e = own_experts * peer_at(table, SEND_ORDER[p]) + core
        cols[p * cand:(p + 1) * cand, :] = lane_column(idx, e)
        at = DONE_SLOT[SEND_ORDER[p]] % pack * cand
        vals[p] = jnp.sum(jnp.where(slot_lane == slot_row + at, lane_column(val, e), 0.0), axis=0, keepdims=True)

    def set_rows(g):
        at = []
        for o in BACK_ORDER[g * COMBINE_PER:(g + 1) * COMBINE_PER]:
            for p in range(n_par):
                at.append(own_experts * peer_at(tables[p], neg(o)) + p)
        n = len(at) * cand
        eye = lax.broadcasted_iota(jnp.int32, (n, n), 0) == lax.broadcasted_iota(jnp.int32, (n, n), 1)
        for source, dst in ((idx, ids), (gate_tab[...], gts)):
            col = jnp.concatenate([lane_column(source, e) for e in at], axis=0)
            dst[g:g + 1, :] = jnp.sum(jnp.where(eye, col, 0.0), axis=0, keepdims=True)

    for p in range(PICK_PER):
        set_columns(p)
    x_copy.wait()

    def gather(g):
        at = pl.multiple_of(g * rows, rows)
        onehot = (lax.broadcasted_iota(jnp.int32, (rows, n_tok), 1).astype(jnp.float32) == cols[pl.ds(at, rows), :]).astype(jnp.bfloat16)
        got = jnp.dot(onehot, x_ref[...], preferred_element_type=jnp.float32).astype(jnp.bfloat16)
        outbox[pl.ds(g * PICK_PER, PICK_PER)] = got.reshape(PICK_PER, cand, d_model)

    half_way = N_CHUNK // 2
    gather(0)
    pl.semaphore_wait(barrier, len(greet))

    def pick(g, c):
        for k in range(1, N_CHUNK):
            @pl.when(g == k)
            def _():
                run_legs(GROUPS[0] + GROUPS[1] if k == 1 else GROUPS[k])
                if k == 1:
                    for w in weights:
                        w.start()
                for p in range(k * PICK_PER, (k + 1) * PICK_PER):
                    if k <= half_way:
                        set_columns(p)
        gather(g)
        for k in range(1, N_CHUNK):
            @pl.when(g == k)
            def _():
                if k == half_way:
                    for p in range((k + 1) * PICK_PER, n_slot):
                        set_columns(p)
                    for o in OFFSETS:
                        val_copy(o).start()
                    gates(cand, logit_ref, idx_tab, gate_tab, soft)
                if k >= half_way:
                    share = N_BACK // (N_CHUNK - half_way)
                    for b in range((k - half_way) * share, (k - half_way + 1) * share):
                        set_rows(b)
        return c

    lax.fori_loop(1, N_CHUNK, pick, 0)
    inbox[DONE_SLOT[SELF]] = outbox[SEND_SLOT[SELF]]
    rval[DONE_SLOT[SELF]] = vals[SEND_SLOT[SELF]]

    def expert(g, c):
        for k in range(N_CHUNK):
            @pl.when(g == k)
            def _():
                run_legs(GROUPS[N_CHUNK + k])
                if k == 0:
                    for o in OFFSETS:
                        val_copy(o).wait_recv()
                    for w in weights:
                        w.wait()
                for o in DONE_ORDER[k * EXPERT_PER:(k + 1) * EXPERT_PER]:
                    if o != SELF:
                        whole(send.at[0], recv.at[LEG_ID[o, N_LEGS[o] - 1]]).wait_recv()
        own = lax.rem(slot_lane, cand) == slot_row
        value = jnp.concatenate([jnp.sum(jnp.where(own, rval[g * EXPERT_PER + i], 0.0), axis=1, keepdims=True) for i in range(EXPERT_PER)], axis=0)

        def count(j, total):
            packed = rval[j * pack]
            for i in range(1, pack):
                packed = packed + rval[j * pack + i]
            return total + (packed > value).astype(jnp.float32)

        above = lax.fori_loop(0, n_slot // pack, count, jnp.zeros((rows, lanes), jnp.float32), unroll=4)
        keep = jnp.sum(above, axis=1, keepdims=True) < float(capacity)
        here = pl.ds(g * EXPERT_PER, EXPERT_PER)
        x = inbox[here].reshape(rows, d_model)
        z = None
        for h in range(2):
            pre = jnp.dot(x, wu[h], preferred_element_type=jnp.float32)
            hid = jax.nn.gelu(pre, approximate=True).astype(jnp.bfloat16)
            term = jnp.dot(hid, wd[h], preferred_element_type=jnp.float32)
            z = term if z is None else z + term
        inbox[here] = jnp.where(keep, z, 0.0).astype(jnp.bfloat16).reshape(EXPERT_PER, cand, d_model)
        return c

    lax.fori_loop(0, N_CHUNK, expert, 0)

    def await_rows(k):
        run_legs(GROUPS[2 * N_CHUNK + k])
        if k == 0:
            for p in range(n_par):
                @pl.when(core == p)
                def _():
                    back[BACK_SLOT[SELF], p] = inbox[DONE_SLOT[SELF], :, p * half:(p + 1) * half]
            split_copy(SELF, inbox.at[DONE_SLOT[SELF]], 1, None).start()
        if k == N_BACK - 1:
            run_legs(GROUPS[2 * N_CHUNK + N_BACK])
        for o in BACK_ORDER[k * COMBINE_PER:(k + 1) * COMBINE_PER]:
            j = BACK_SLOT[o]
            if o != SELF:
                part(asend.at[j], arecv.at[j]).wait_recv()
            part(bsend.at[j], brecv.at[j]).wait_recv()

    def gated_sum(g, first, count):
        n = ids.shape[1]
        z = back[pl.ds(g * COMBINE_PER, COMBINE_PER)].reshape(n, half)
        token = lax.broadcasted_iota(jnp.int32, (count, n), 0) + first
        hit = token.astype(jnp.float32) == ids[pl.ds(g, 1), :]
        left = gts[pl.ds(g, 1), :]
        total = None
        for _ in range(3):
            piece = left.astype(jnp.bfloat16)
            left = left - piece.astype(jnp.float32)
            mat = jnp.where(hit, piece.astype(jnp.float32), 0.0).astype(jnp.bfloat16)
            term = jnp.dot(mat, z, preferred_element_type=jnp.float32)
            total = term if total is None else total + term
        return total

    def combine(g, c):
        for k in range(N_BACK - 1):
            @pl.when(g == k)
            def _():
                await_rows(k)
        total = gated_sum(g, 0, n_tok)

        @pl.when(g == 0)
        def _():
            acc[...] = total

        @pl.when(g > 0)
        def _():
            acc[...] += total
        return c

    lax.fori_loop(0, N_BACK - 1, combine, 0)
    await_rows(N_BACK - 1)
    n_part = osend.shape[0]
    size = n_tok // n_part

    def out_copies(b):
        at = pl.ds(pl.multiple_of(b * size, size), size)
        half_of = out_ref.at[at, mine]
        return (pltpu.make_async_remote_copy(half_of, half_of, osend.at[b], orecv.at[b], device_id={"tp": other}, device_id_type=MESH),)

    def finish(b, c):
        at = pl.ds(pl.multiple_of(b * size, size), size)
        y = acc[at, :] + gated_sum(N_BACK - 1, b * size, size)
        for p in range(n_par):
            @pl.when(core == p)
            def _():
                out_ref[at, p * half:(p + 1) * half] = (x_ref[at, p * half:(p + 1) * half].astype(jnp.float32) + y).astype(jnp.bfloat16)
        for copy in out_copies(b):
            copy.start()
        return c

    lax.fori_loop(0, n_part, finish, 0)

    def drain_legs(k, c):
        whole(send.at[k], recv.at[0]).wait_send()
        return c

    lax.fori_loop(0, len(OUT_LEGS), drain_legs, 0)

    def drain_vals(j, c):
        pltpu.make_async_remote_copy(rval.at[0], rval.at[0], vsend.at[j], vrecv.at[0], device_id={"tp": other}, device_id_type=MESH).wait_send()
        return c

    lax.fori_loop(0, len(OFFSETS), drain_vals, 0)
    for _, o, _, i in BACK_LEGS:
        if i < N_LEGS[o] - 1:
            whole(rsend.at[BACK_ID[o, i]], rrecv.at[0]).wait_send()

    def drain_back(j, c):
        @pl.when(j != BACK_SLOT[SELF])
        def _():
            part(asend.at[j], arecv.at[j]).wait_send()
        part(bsend.at[j], brecv.at[j]).wait_send()
        return c

    lax.fori_loop(0, n_slot, drain_back, 0)

    def drain_out(b, c):
        for copy in out_copies(b):
            copy.wait()
        return c

    lax.fori_loop(0, n_part, drain_out, 0)


def solution(mesh):
    n_groups = mesh.shape["ep"]
    any_spec = pl.BlockSpec(memory_space=pl.ANY)
    vmem_spec = pl.BlockSpec(memory_space=pltpu.VMEM)
    dma = pltpu.SemaphoreType.DMA
    n_legs, n_jobs = len(OUT_LEGS), len(OFFSETS)

    def local_layer(x_local, logit_local, w_up, w_down):
        n_tok, d_model = x_local.shape
        n_experts = logit_local.shape[1]
        own_experts, _, hid = w_up.shape
        capacity = CAP_FACTOR * n_tok * n_groups // n_experts
        cand = 2 * capacity // n_groups
        half = d_model // 2
        n_back_rows = COMBINE_PER * own_experts * cand
        block = lambda n: pltpu.VMEM((n, cand, d_model), jnp.bfloat16)
        table = pltpu.VMEM((cand, n_experts), jnp.float32)
        score = pltpu.VMEM((n_tok, n_experts), jnp.float32)

        out, _, _ = pl.pallas_call(
            functools.partial(layer_kernel, capacity),
            out_shape=(
                pltpu.VMEM((n_tok, d_model), jnp.bfloat16),
                jax.ShapeDtypeStruct((N_HOP[0], cand, d_model), jnp.bfloat16),
                jax.ShapeDtypeStruct((N_HOP[1], cand, d_model), jnp.bfloat16),
            ),
            in_specs=[vmem_spec, any_spec, any_spec, any_spec],
            out_specs=(vmem_spec, any_spec, any_spec),
            scratch_shapes=[
                pltpu.VMEM((n_tok, d_model), jnp.bfloat16),
                table, table, table, score, score,
                pltpu.VMEM((n_groups, 1, 128), jnp.float32),
                pltpu.VMEM((n_groups * cand, 1), jnp.float32),
                pltpu.VMEM((N_BACK, n_back_rows), jnp.float32), pltpu.VMEM((N_BACK, n_back_rows), jnp.float32),
                block(n_groups), block(N_HOP[0]), block(N_HOP[1]), block(n_groups),
                pltpu.VMEM((n_groups, 1, 128), jnp.float32),
                pltpu.VMEM((2, d_model, hid), jnp.bfloat16), pltpu.VMEM((2, hid, d_model), jnp.bfloat16),
                pltpu.VMEM((n_groups, own_experts, cand, half), jnp.bfloat16),
                pltpu.VMEM((n_tok, half), jnp.float32),
                dma((n_legs,)), dma((n_legs,)), dma((n_jobs,)), dma((n_jobs,)), dma((2,)), dma((2,)), dma((2,)),
                dma((n_legs,)), dma((n_legs,)), dma((n_groups,)), dma((n_groups,)), dma((n_groups,)), dma((n_groups,)),
                dma((4,)), dma((4,)), dma,
            ],
            compiler_params=pltpu.CompilerParams(collective_id=0, has_side_effects=True, vmem_limit_bytes=VMEM_LIMIT),
        )(logit_local, x_local, w_up, w_down)
        return out

    token_spec = P(("dp", "ep"), None)
    return jax.shard_map(local_layer, mesh=mesh, in_specs=(token_spec, token_spec, P("ep", None, "tp"), P("ep", "tp", None)), out_specs=token_spec, check_vma=False)
```
